256 devices in a mesh: tm: 32 (over y_hi, z, core), asset: 8 (over x, y_lo).
Axes of the slice: x: 4, y: 4 (y_hi: 2, y_lo: 2; y = y_hi * 2 + y_lo), z: 8, core: 2. Of those that a mesh axis runs over, the one named last changes fastest.
Arguments:
- returns: bfloat16 [128, 8192], P('tm', 'asset'), as said below
- signal: bfloat16 [128, 8192], P('tm', 'asset'), may hold values from -6 to 6
- earlier: bfloat16 [59, 8192], P(None, 'asset'), as said below
Outputs:
- filtered: float32 [128, 8192], P('tm', 'asset')
The draws below stay inside these ranges and needn't reach their ends.
Inputs may be any that keep to these rules, and one draw needn't show every extreme that they name: Each equity has its own scale of returns, the same in returns and earlier. `earlier`: drawn by the same law as returns, with the same scale for each equity.
All inputs are finite; a program needn't handle non-finite values.
Results may differ from the reference program's by a relative error of at most 0.0032.
Values may be sent and summed in bfloat16 or wider, within the bound.
A program may use at most 64 MiB of HBM per device.

```python
import jax
import jax.numpy as jnp
from jax import lax

ASSETS = 8192
WIN = 60
HIST = 59
DAYS = 128


def asset_scales(key):
    sub_key = jax.random.fold_in(key, 7)
    return jnp.exp(jax.random.uniform(sub_key, (ASSETS,), jnp.float32, jnp.log(0.1), jnp.log(3.0)))


def draw_rows(key, salt, count):
    scales = asset_scales(key)
    noise_key = jax.random.fold_in(key, salt)
    values = jnp.clip(jax.random.normal(noise_key, (count, ASSETS), jnp.float32), -6.0, 6.0)
    return (values * scales[None, :]).astype(jnp.bfloat16)


def draw_returns(key, part):
    return draw_rows(key, 11, DAYS)


def draw_earlier(key, part):
    return draw_rows(key, 13, HIST)


def level_of(own_key, extent, shards, low, largest):
    loudness = 1.0
    for axis_at, shards_of in shards:
        heights = jax.random.uniform(jax.random.fold_in(jax.random.fold_in(own_key, 6), axis_at), (shards_of,), jnp.float32, low / len(shards), largest / len(shards))
        loudness = loudness * jnp.repeat(jnp.exp(heights), extent[axis_at] // shards_of).reshape((-1,) + (1,) * (len(extent) - 1 - axis_at))
    return loudness


def scatter_about(own_key, shape, deviation, bound, shards=(), kind=jnp.bfloat16):
    gain = level_of(own_key, shape, shards, -0.22, 0.18) if shards else 1.0
    drawn = jax.random.normal(own_key, shape, jnp.float32) * deviation * gain
    return jnp.minimum(jnp.maximum(drawn, -bound), bound).astype(kind)


def setup_inputs(seed: int = 0) -> dict:
    keys = jax.random.split(jax.random.key(seed), 4)
    returns = draw_returns(jax.random.fold_in(keys[3], 71), 0)
    signal = scatter_about(keys[1], (DAYS, ASSETS), 1.0, 6.0, ((0, 32), (1, 8)))
    earlier = draw_earlier(jax.random.fold_in(keys[3], 71), 0)
    return {"returns": returns, "signal": signal, "earlier": earlier}


var_floor = 0.05
shrink_level = 0.1

def moments(window):
    values = window.astype(jnp.float32)
    center = lax.optimization_barrier(jnp.mean(values, axis=0))
    spread = lax.optimization_barrier(jnp.mean(values * values, axis=0)) - center * center
    return (center, jnp.sqrt(jnp.maximum(spread, var_floor)))

def contribution(ext_rows, ext_cols, signal_cols):

    def one_day(day_index):
        window_rows = lax.dynamic_slice_in_dim(ext_rows, day_index, WIN, 0)
        window_cols = lax.dynamic_slice_in_dim(ext_cols, day_index, WIN, 0)
        mean_rows, scale_rows = moments(window_rows)
        mean_cols, scale_cols = moments(window_cols)
        gram_tile = lax.dot_general(window_rows, window_cols, (((0,), (0,)), ((), ())), preferred_element_type=jnp.float32)
        correlation = (gram_tile / WIN - mean_rows[:, None] * mean_cols[None, :]) / (scale_rows[:, None] * scale_cols[None, :])
        shrunk = (jnp.sign(correlation) * jnp.maximum(jnp.abs(correlation) - shrink_level, 0.0)).astype(jnp.bfloat16)
        day_signal = lax.dynamic_index_in_dim(signal_cols, day_index, 0, keepdims=False)
        return jnp.dot(shrunk, day_signal, preferred_element_type=jnp.float32)
    return lax.map(one_day, jnp.arange(signal_cols.shape[0], dtype=jnp.int32))

def reference(returns, signal, earlier):
    extended = jnp.concatenate([earlier, returns], 0)
    row_block = min(ASSETS, 1024)
    blocks_count = ASSETS // row_block

    def row_part(block_index):
        own_rows = lax.dynamic_slice_in_dim(extended, block_index * row_block, row_block, 1)
        return contribution(own_rows, extended, signal)
    stacked = lax.map(row_part, jnp.arange(blocks_count, dtype=jnp.int32))
    return jnp.transpose(stacked, (1, 0, 2)).reshape(DAYS, ASSETS)
```

```python
import jax
import jax.numpy as jnp
from jax import lax
from jax.experimental import pallas as pl
from jax.experimental.pallas import tpu as pltpu
from jax.sharding import PartitionSpec as P

WIN = 60
HIST = 59
DEPTH = 64
TILE = 256
STRIP = 128
LAG = 4

var_floor = 0.05
shrink_level = 0.1


def passed_along(value, axis, by):
    peers = lax.axis_size(axis)
    pairs = [(i, i + by) for i in range(peers) if 0 <= i + by < peers]
    return lax.ppermute(value, axis, pairs)


def history(block_rows, earlier_rows):
    day_dev = block_rows.shape[0]
    position = lax.axis_index("tm")
    span = HIST + day_dev
    blocks_needed = -(-HIST // day_dev)
    stacked = block_rows
    for level in range(blocks_needed.bit_length()):
        moved = passed_along(stacked, "tm", 1 << level)
        stacked = jnp.concatenate([moved, stacked], 0)
    tail_rows = stacked[stacked.shape[0] - span :]
    padded = jnp.concatenate(
        [earlier_rows, jnp.zeros((span, earlier_rows.shape[1]), earlier_rows.dtype)], 0
    )
    filler = lax.dynamic_slice_in_dim(padded, position * day_dev, span, 0)
    offsets = position * day_dev - HIST + jnp.arange(span, dtype=jnp.int32)
    return jnp.where((offsets < 0)[:, None], filler, tail_rows)


def totals(x):
    middle = x[8:16]
    middle_sq = middle * middle
    for at in range(16, DEPTH - 8, 8):
        part = x[at : at + 8]
        middle = middle + part
        middle_sq = middle_sq + part * part
    return middle, middle_sq


def day_edges(x, day):
    row = lax.broadcasted_iota(jnp.int32, (8, x.shape[1]), 0)
    first = jnp.where(row >= day, x[:8], 0.0)
    last = jnp.where(row <= day + (WIN - 1 - (DEPTH - 8)), x[DEPTH - 8 :], 0.0)
    return first, last


def day_moments(x, middle, middle_sq, day):
    first, last = day_edges(x, day)
    total = jnp.sum(middle + first + last, axis=0, keepdims=True)
    total_sq = jnp.sum(middle_sq + first * first + last * last, axis=0, keepdims=True)
    center = total * (1.0 / WIN)
    spread = total_sq * (1.0 / WIN) - center * center
    return center, lax.rsqrt(jnp.maximum(spread, var_floor))


def day_values(x, center, factor, day):
    row = lax.broadcasted_iota(jnp.int32, (8, x.shape[1]), 0)
    scaled = (x - center) * factor
    first = jnp.where(row >= day, scaled[:8], 0.0)
    last = jnp.where(row <= day + (WIN - 1 - (DEPTH - 8)), scaled[DEPTH - 8 :], 0.0)
    return jnp.concatenate([first, scaled[8 : DEPTH - 8], last], 0)


def halves(x):
    high = x.astype(jnp.bfloat16)
    low = (x - high.astype(jnp.float32)).astype(jnp.bfloat16)
    return high, low


def kernel(own_ref, all_ref, out_ref, high_ref, low_ref, bound_ref, lhs_ref, row_ref, sum_ref, lin_ref):
    days = out_ref.shape[0]
    mine = own_ref.shape[1]
    blocks, width = all_ref.shape[0], all_ref.shape[2]
    per_block = width // TILE
    tiles = blocks * per_block

    for at in range(0, mine, TILE):
        x = own_ref[:DEPTH, at : at + TILE].astype(jnp.float32)
        middle, middle_sq = totals(x)
        for day in range(days):
            center, inverse = day_moments(x, middle, middle_sq, day)
            w = day_values(x, center, inverse * (1.0 / (WIN * shrink_level)), day)
            row_ref[day, :, at : at + TILE] = w
            high = w.astype(jnp.bfloat16).astype(jnp.float32)
            both = jnp.concatenate([high, w - high], 0)
            for sub in range(0, TILE, 128):
                turned = both[:, sub : sub + 128].T.astype(jnp.bfloat16)
                lhs_ref[day, at + sub : at + sub + 128, :128] = turned
                lhs_ref[day, at + sub : at + sub + 128, 128:] = turned

    lin_ref[...] = jnp.zeros_like(lin_ref)

    def prepare(block, carry):
        for sub in range(per_block):
            cols = pl.ds(sub * TILE, TILE)
            dst = block * per_block + sub
            x = all_ref[block, :DEPTH, cols].astype(jnp.float32)
            signal = all_ref[block, DEPTH : DEPTH + days, cols].astype(jnp.float32)
            middle, middle_sq = totals(x)
            for day in range(days):
                s = signal[day : day + 1]
                center, inverse = day_moments(x, middle, middle_sq, day)
                v = day_values(x, center, inverse * s, day)
                lin_ref[day] += v[:, :128] + v[:, 128:]
                high, low = halves(v)
                high_ref[day, dst] = high
                low_ref[day, dst] = low
                bound_ref[day, dst] = jnp.broadcast_to(jnp.abs(s), (8, TILE))
        return carry

    lax.fori_loop(0, blocks, prepare, 0)

    def compute(*accs):
        per_unit = mine // STRIP

        def one_day(day, carry):
            def take(step):
                pair, strip = divmod(step, per_unit)
                rows = pl.ds(strip * STRIP, STRIP)
                part = None
                for unit in range(2):
                    bound = bound_ref[day, 2 * pair + unit][:1]
                    got = pltpu.matmul_pop(accs[unit * per_unit + strip])
                    kept = jnp.minimum(jnp.maximum(got, -bound), bound)
                    kept = kept[:, :128] + kept[:, 128:]
                    part = kept if part is None else part + kept
                if pair == 0:
                    sum_ref[rows, :] = part
                else:
                    sum_ref[rows, :] += part

            steps = tiles // 2 * per_unit
            for step in range(steps):
                pair, strip = divmod(step, per_unit)
                if strip == 0:
                    for unit in range(2):
                        high = high_ref[day, 2 * pair + unit]
                        low = low_ref[day, 2 * pair + unit]
                        pltpu.matmul_push_rhs(
                            jnp.concatenate([high, high, low, low], 0),
                            staging_register=pair % 2,
                            mxu_index=unit,
                        )
                lhs = lhs_ref[day, strip * STRIP : (strip + 1) * STRIP, :]
                for unit in range(2):
                    pltpu.matmul_acc_lhs(
                        accs[unit * per_unit + strip],
                        lhs,
                        load_staged_rhs=pair % 2 if strip == 0 else None,
                    )
                if step >= LAG:
                    take(step - LAG)
            for step in range(steps - LAG, steps):
                take(step)

            weight = jnp.sum(lin_ref[day], axis=1, keepdims=True)
            line = jnp.sum(row_ref[day] * weight, axis=0, keepdims=True)
            clamped = jnp.concatenate(
                [
                    jnp.sum(sum_ref[at : at + 128, :].T, axis=0, keepdims=True)
                    for at in range(0, mine, 128)
                ],
                1,
            )
            out_ref[pl.ds(day, 1), :] = (line - clamped) * shrink_level
            return carry

        lax.fori_loop(0, days, one_day, 0)

    strips = mine // STRIP
    pl.run_scoped(
        compute,
        *[pltpu.ACC(unit)((STRIP, TILE), jnp.float32) for unit in range(2) for _ in range(strips)],
    )


def filtered_rows(own, everyone, days):
    mine = own.shape[1]
    blocks, _, width = everyone.shape
    tiles = blocks * width // TILE
    vmem = pl.BlockSpec(memory_space=pltpu.VMEM)
    return pl.pallas_call(
        kernel,
        out_shape=jax.ShapeDtypeStruct((days, mine), jnp.float32),
        in_specs=[vmem, vmem],
        out_specs=vmem,
        scratch_shapes=[
            pltpu.VMEM((days, tiles, DEPTH, TILE), jnp.bfloat16),
            pltpu.VMEM((days, tiles, DEPTH, TILE), jnp.bfloat16),
            pltpu.VMEM((days, tiles, 8, TILE), jnp.float32),
            pltpu.VMEM((days, mine, TILE), jnp.bfloat16),
            pltpu.VMEM((days, DEPTH, mine), jnp.float32),
            pltpu.VMEM((mine, 128), jnp.float32),
            pltpu.VMEM((days, DEPTH, 128), jnp.float32),
        ],
        compiler_params=pltpu.CompilerParams(vmem_limit_bytes=48 << 20),
        name="filter_days",
    )(own, everyone)


def per_device(returns, signal, earlier):
    days = returns.shape[0]
    extended = history(returns, earlier)
    blank = jnp.zeros((DEPTH - extended.shape[0], extended.shape[1]), extended.dtype)
    own = jnp.concatenate([extended, blank, signal], 0)
    copies = jnp.broadcast_to(own, (lax.axis_size("asset"), *own.shape))
    everyone = lax.all_to_all(copies, "asset", split_axis=0, concat_axis=0, tiled=True)
    return filtered_rows(own, everyone, days)


def solution(mesh):
    in_specs = (P("tm", "asset"), P("tm", "asset"), P(None, "asset"))
    out_specs = P("tm", "asset")
    return jax.shard_map(
        per_device, mesh=mesh, in_specs=in_specs, out_specs=out_specs, check_vma=False
    )
```

```python
import jax
import jax.numpy as jnp
from jax import lax
from jax.experimental import pallas as pl
from jax.experimental.pallas import tpu as pltpu
from jax.sharding import PartitionSpec as P

WIN = 60
HIST = 59
DEPTH = 64
TILE = 256
STRIP = 128
LAG = 4
BLOCKS = 16

var_floor = 0.05
shrink_level = 0.1


def odd_place(slot):
    return 1 + slot // 2


def even_place(slot):
    return 9 + slot // 2


def gather_kernel(returns_ref, signal_ref, old_ref, out_ref, send_far, got_far, send_peer, got_peer, send_edge, got_edge, send_twin, got_twin):
    time, own = lax.axis_index("tm"), lax.axis_index("asset")
    times, peers = lax.axis_size("tm"), lax.axis_size("asset")
    core = lax.rem(time, 2)
    twin = time + 1 - 2 * core
    even, odd = core == 0, core == 1
    reach = BLOCKS - 1

    def peer(step):
        return lax.rem(own + step, peers)

    def at(t, a):
        return dict(device_id=(t, a), device_id_type=pl.DeviceIdType.MESH)

    barrier = pltpu.get_barrier_semaphore()

    def greet(valid, t, a):
        @pl.when(valid)
        def _():
            pl.semaphore_signal(barrier, inc=1, **at(t, a))

    count = peers
    for back in range(2, reach, 2):
        greet(time + back < times, time + back, own)
        greet(time - back >= 0, time - back, own)
        count += (time + back < times).astype(jnp.int32) + (time - back >= 0).astype(jnp.int32)
    forward = jnp.logical_and(odd, time + reach < times)
    backward = jnp.logical_and(even, time - reach >= 0)
    greet(forward, time + reach, own)
    greet(backward, time - reach, own)
    count += forward.astype(jnp.int32) + backward.astype(jnp.int32)
    for step in range(1, peers):
        pl.semaphore_signal(barrier, inc=1, **at(time, peer(step)))
    pl.semaphore_signal(barrier, inc=1, **at(twin, own))
    pl.semaphore_wait(barrier, count)

    def far(back, place, to):
        return pltpu.make_async_remote_copy(
            src_ref=returns_ref,
            dst_ref=out_ref.at[own, place],
            send_sem=send_far.at[back // 2],
            recv_sem=got_far.at[back // 2],
            **at(to, own),
        )

    for back in range(2, reach, 2):
        @pl.when(time + back < times)
        def _(back=back):
            far(back, odd_place(reach - back), time + back).start()

    @pl.when(forward)
    def _():
        pltpu.make_async_remote_copy(
            src_ref=returns_ref,
            dst_ref=out_ref.at[own, even_place(0)],
            send_sem=send_far.at[0],
            recv_sem=got_far.at[0],
            **at(time + reach, own),
        ).start()

    out_ref[own, 0] = signal_ref[...]
    out_ref[own, odd_place(reach)] = returns_ref[...]
    for slot in range(1, reach, 2):
        @pl.when(time + slot < reach)
        def _(slot=slot):
            out_ref[own, odd_place(slot)] = old_ref[time + slot]

    @pl.when(jnp.logical_and(even, time < reach))
    def _():
        out_ref[own, even_place(0)] = old_ref[time]

    for back in range(2, reach, 2):
        @pl.when(time - back >= 0)
        def _(back=back):
            far(back, odd_place(reach - back), time).wait_recv()

        @pl.when(time + back < times)
        def _(back=back):
            far(back, odd_place(reach - back), time).wait_send()

    def edge_far():
        return pltpu.make_async_remote_copy(
            src_ref=returns_ref,
            dst_ref=out_ref.at[own, even_place(0)],
            send_sem=send_far.at[0],
            recv_sem=got_far.at[0],
            **at(time, own),
        )

    @pl.when(backward)
    def _():
        edge_far().wait_recv()

    @pl.when(forward)
    def _():
        edge_far().wait_send()

    half = pl.ds(0, 9)

    def across(step, a):
        return pltpu.make_async_remote_copy(
            src_ref=out_ref.at[a, half],
            dst_ref=out_ref.at[a, half],
            send_sem=send_peer.at[step],
            recv_sem=got_peer.at[step],
            **at(time, peer(step)),
        )

    def across_edge(step, a):
        return pltpu.make_async_remote_copy(
            src_ref=out_ref.at[a, even_place(0)],
            dst_ref=out_ref.at[a, even_place(0)],
            send_sem=send_edge.at[step],
            recv_sem=got_edge.at[step],
            **at(time, peer(step)),
        )

    def over(step, a, low):
        size = 7 + low
        return pltpu.make_async_remote_copy(
            src_ref=out_ref.at[a, pl.ds(1, size)],
            dst_ref=out_ref.at[a, pl.ds(10 - low, size)],
            send_sem=send_twin.at[step],
            recv_sem=got_twin.at[step],
            **at(twin, own),
        )

    for step in range(1, peers):
        across(step, own).start()

        @pl.when(even)
        def _(step=step):
            across_edge(step, own).start()

    def hand_over(step, a):
        @pl.when(even)
        def _():
            over(step, a, 1).start()

        @pl.when(odd)
        def _():
            over(step, a, 0).start()

    hand_over(0, own)
    for step in range(1, peers):
        source = peer(peers - step)
        across(step, source).wait_recv()
        hand_over(step, source)

    for step in range(peers):
        source = peer(peers - step)

        @pl.when(even)
        def _(step=step, source=source):
            over(step, source, 0).wait_recv()
            over(step, source, 1).wait_send()

        @pl.when(odd)
        def _(step=step, source=source):
            over(step, source, 1).wait_recv()
            over(step, source, 0).wait_send()

        if step:
            across(step, own).wait_send()

            @pl.when(even)
            def _(step=step, source=source):
                across_edge(step, source).wait_recv()
                across_edge(step, own).wait_send()


def gathered(returns, signal, earlier):
    days, mine = returns.shape
    peers = lax.axis_size("asset")
    old = jnp.pad(earlier, ((1, 0), (0, 0))).reshape(BLOCKS - 1, days, mine)
    vmem = pl.BlockSpec(memory_space=pltpu.VMEM)
    dma = pltpu.SemaphoreType.DMA
    return pl.pallas_call(
        gather_kernel,
        out_shape=jax.ShapeDtypeStruct((peers, BLOCKS + 1, days, mine), returns.dtype),
        in_specs=[vmem] * 3,
        out_specs=vmem,
        scratch_shapes=[dma((BLOCKS // 2,))] * 2 + [dma((peers,))] * 6,
        compiler_params=pltpu.CompilerParams(
            collective_id=0, has_side_effects=True, vmem_limit_bytes=8 << 20
        ),
        name="gather_windows",
    )(returns, signal, old)


def totals(x):
    middle = middle_sq = None
    for at in range(0, DEPTH, 8):
        if at in (24, 32):
            continue
        part = x[at : at + 8]
        middle = part if middle is None else middle + part
        middle_sq = part * part if middle_sq is None else middle_sq + part * part
    return middle, middle_sq


def day_edges(x, day):
    row = lax.broadcasted_iota(jnp.int32, (8, x.shape[1]), 0)
    newest = jnp.where(row <= day + 4, x[24:32], 0.0)
    oldest = jnp.where(row >= day + 1, x[32:40], 0.0)
    return newest, oldest


def day_moments(x, middle, middle_sq, day):
    newest, oldest = day_edges(x, day)
    total = jnp.sum(middle + newest + oldest, axis=0, keepdims=True)
    total_sq = jnp.sum(middle_sq + newest * newest + oldest * oldest, axis=0, keepdims=True)
    center = total * (1.0 / WIN)
    spread = total_sq * (1.0 / WIN) - center * center
    return center, lax.rsqrt(jnp.maximum(spread, var_floor))


def day_values(x, center, factor, day):
    scaled = (x - center) * factor
    newest, oldest = day_edges(scaled, day)
    return jnp.concatenate([scaled[:24], newest, oldest, scaled[40:]], 0)


def halves(x):
    high = x.astype(jnp.bfloat16)
    low = (x - high.astype(jnp.float32)).astype(jnp.bfloat16)
    return high, low


def window(all_ref, block, cols):
    x = all_ref[block, 1:, :, cols].astype(jnp.float32)
    return x.reshape(DEPTH, TILE)


def kernel(all_ref, out_ref, high_ref, low_ref, bound_ref, lhs_ref, row_ref, sum_ref, lin_ref):
    days = out_ref.shape[0]
    blocks, width = all_ref.shape[0], all_ref.shape[3]
    mine = width
    own = lax.axis_index("asset")
    per_block = width // TILE
    tiles = blocks * per_block

    for at in range(0, mine, TILE):
        x = window(all_ref, own, pl.ds(at, TILE))
        middle, middle_sq = totals(x)
        for day in range(days):
            center, inverse = day_moments(x, middle, middle_sq, day)
            w = day_values(x, center, inverse * (1.0 / (WIN * shrink_level)), day)
            row_ref[day, :, at : at + TILE] = w
            high = w.astype(jnp.bfloat16).astype(jnp.float32)
            both = jnp.concatenate([high, w - high], 0)
            for sub in range(0, TILE, 128):
                turned = both[:, sub : sub + 128].T.astype(jnp.bfloat16)
                lhs_ref[day, at + sub : at + sub + 128, :128] = turned
                lhs_ref[day, at + sub : at + sub + 128, 128:] = turned

    lin_ref[...] = jnp.zeros_like(lin_ref)

    def prepare(block, carry):
        for sub in range(per_block):
            cols = pl.ds(sub * TILE, TILE)
            dst = block * per_block + sub
            x = window(all_ref, block, cols)
            signal = all_ref[block, 0, :, cols].astype(jnp.float32)
            middle, middle_sq = totals(x)
            for day in range(days):
                s = signal[day : day + 1]
                center, inverse = day_moments(x, middle, middle_sq, day)
                v = day_values(x, center, inverse * s, day)
                lin_ref[day] += v[:, :128] + v[:, 128:]
                high, low = halves(v)
                high_ref[day, dst] = high
                low_ref[day, dst] = low
                bound_ref[day, dst] = jnp.broadcast_to(jnp.abs(s), (8, TILE))
        return carry

    lax.fori_loop(0, blocks, prepare, 0)

    def compute(*accs):
        per_unit = mine // STRIP

        def one_day(day, carry):
            def take(step):
                pair, strip = divmod(step, per_unit)
                rows = pl.ds(strip * STRIP, STRIP)
                part = None
                for unit in range(2):
                    bound = bound_ref[day, 2 * pair + unit][:1]
                    got = pltpu.matmul_pop(accs[unit * per_unit + strip])
                    kept = jnp.minimum(jnp.maximum(got, -bound), bound)
                    kept = kept[:, :128] + kept[:, 128:]
                    part = kept if part is None else part + kept
                if pair == 0:
                    sum_ref[rows, :] = part
                else:
                    sum_ref[rows, :] += part

            steps = tiles // 2 * per_unit
            for step in range(steps):
                pair, strip = divmod(step, per_unit)
                if strip == 0:
                    for unit in range(2):
                        high = high_ref[day, 2 * pair + unit]
                        low = low_ref[day, 2 * pair + unit]
                        pltpu.matmul_push_rhs(
                            jnp.concatenate([high, high, low, low], 0),
                            staging_register=pair % 2,
                            mxu_index=unit,
                        )
                lhs = lhs_ref[day, strip * STRIP : (strip + 1) * STRIP, :]
                for unit in range(2):
                    pltpu.matmul_acc_lhs(
                        accs[unit * per_unit + strip],
                        lhs,
                        load_staged_rhs=pair % 2 if strip == 0 else None,
                    )
                if step >= LAG:
                    take(step - LAG)
            for step in range(steps - LAG, steps):
                take(step)

            weight = jnp.sum(lin_ref[day], axis=1, keepdims=True)
            line = jnp.sum(row_ref[day] * weight, axis=0, keepdims=True)
            clamped = jnp.concatenate(
                [
                    jnp.sum(sum_ref[at : at + 128, :].T, axis=0, keepdims=True)
                    for at in range(0, mine, 128)
                ],
                1,
            )
            out_ref[pl.ds(day, 1), :] = (line - clamped) * shrink_level
            return carry

        lax.fori_loop(0, days, one_day, 0)

    strips = mine // STRIP
    pl.run_scoped(
        compute,
        *[pltpu.ACC(unit)((STRIP, TILE), jnp.float32) for unit in range(2) for _ in range(strips)],
    )


def filtered_rows(everyone):
    blocks, _, days, width = everyone.shape
    mine = width
    tiles = blocks * width // TILE
    vmem = pl.BlockSpec(memory_space=pltpu.VMEM)
    return pl.pallas_call(
        kernel,
        out_shape=jax.ShapeDtypeStruct((days, mine), jnp.float32),
        in_specs=[vmem],
        out_specs=vmem,
        scratch_shapes=[
            pltpu.VMEM((days, tiles, DEPTH, TILE), jnp.bfloat16),
            pltpu.VMEM((days, tiles, DEPTH, TILE), jnp.bfloat16),
            pltpu.VMEM((days, tiles, 8, TILE), jnp.float32),
            pltpu.VMEM((days, mine, TILE), jnp.bfloat16),
            pltpu.VMEM((days, DEPTH, mine), jnp.float32),
            pltpu.VMEM((mine, 128), jnp.float32),
            pltpu.VMEM((days, DEPTH, 128), jnp.float32),
        ],
        compiler_params=pltpu.CompilerParams(vmem_limit_bytes=48 << 20),
        name="filter_days",
    )(everyone)


def per_device(returns, signal, earlier):
    return filtered_rows(gathered(returns, signal, earlier))


def solution(mesh):
    in_specs = (P("tm", "asset"), P("tm", "asset"), P(None, "asset"))
    out_specs = P("tm", "asset")
    return jax.shard_map(
        per_device, mesh=mesh, in_specs=in_specs, out_specs=out_specs, check_vma=False
    )
```

```python
import jax
import jax.numpy as jnp
from jax import lax
from jax.experimental import pallas as pl
from jax.experimental.pallas import tpu as pltpu
from jax.sharding import PartitionSpec as P

WIN = 60
HIST = 59
DEPTH = 64
TILE = 256
STRIP = 128
LAG = 4
BLOCKS = 16

var_floor = 0.05
shrink_level = 0.1


def totals(x):
    middle = middle_sq = None
    for at in range(0, DEPTH, 8):
        if at in (24, 32):
            continue
        part = x[at : at + 8]
        middle = part if middle is None else middle + part
        middle_sq = part * part if middle_sq is None else middle_sq + part * part
    return middle, middle_sq


def day_edges(x, day):
    row = lax.broadcasted_iota(jnp.int32, (8, x.shape[1]), 0)
    newest = jnp.where(row <= day + 4, x[24:32], 0.0)
    oldest = jnp.where(row >= day + 1, x[32:40], 0.0)
    return newest, oldest


def day_moments(x, middle, middle_sq, day):
    newest, oldest = day_edges(x, day)
    total = jnp.sum(middle + newest + oldest, axis=0, keepdims=True)
    total_sq = jnp.sum(middle_sq + newest * newest + oldest * oldest, axis=0, keepdims=True)
    center = total * (1.0 / WIN)
    spread = total_sq * (1.0 / WIN) - center * center
    return center, lax.rsqrt(jnp.maximum(spread, var_floor))


def day_values(x, center, factor, day):
    scaled = (x - center) * factor
    newest, oldest = day_edges(scaled, day)
    return jnp.concatenate([scaled[:24], newest, oldest, scaled[40:]], 0)


def halves(x):
    high = x.astype(jnp.bfloat16)
    low = (x - high.astype(jnp.float32)).astype(jnp.bfloat16)
    return high, low


def odd_place(slot):
    return 1 + slot // 2


def even_place(slot):
    return 9 + slot // 2


def window(store_ref, block, cols):
    x = store_ref[block, 1:, :, cols].astype(jnp.float32)
    return x.reshape(DEPTH, TILE)


def kernel(
    returns_ref, signal_ref, earlier_ref, out_ref,
    store_ref, old_ref, before_ref, high_ref, low_ref, bound_ref, lhs_ref, row_ref, sum_ref, lin_ref, x_ref, tot_ref,
    fill_sem, send_far, got_far, send_peer, got_peer, send_edge, got_edge, send_twin, got_twin,
):
    days, mine = out_ref.shape
    time, own = lax.axis_index("tm"), lax.axis_index("asset")
    times, peers = lax.axis_size("tm"), lax.axis_size("asset")
    core = lax.rem(time, 2)
    twin = time + 1 - 2 * core
    even, odd = core == 0, core == 1
    reach = BLOCKS - 1
    column, side = own // 2, lax.rem(own, 2)

    def at(t, a):
        return dict(device_id=(t, a), device_id_type=pl.DeviceIdType.MESH)

    def peer(step, sign):
        along = (0, 0, 1, 3, 2, 1, 3, 2)[step]
        other = (0, 1, 0, 0, 0, 1, 1, 1)[step]
        flipped = 1 - side if other else side
        return 2 * lax.rem(column + (along if sign > 0 else peers // 2 - along), peers // 2) + flipped

    fills = [
        pltpu.make_async_copy(returns_ref, store_ref.at[0, odd_place(reach)], fill_sem.at[0]),
        pltpu.make_async_copy(signal_ref, store_ref.at[0, 0], fill_sem.at[1]),
        pltpu.make_async_copy(earlier_ref, before_ref, fill_sem.at[2]),
    ]
    for fill in fills:
        fill.start()

    barrier = pltpu.get_barrier_semaphore()

    def greet(valid, t, a):
        @pl.when(valid)
        def _():
            pl.semaphore_signal(barrier, inc=1, **at(t, a))

    count = peers
    forward = jnp.logical_and(odd, time + reach < times)
    backward = jnp.logical_and(even, time - reach >= 0)
    greet(forward, time + reach, own)
    greet(backward, time - reach, own)
    count += forward.astype(jnp.int32) + backward.astype(jnp.int32)
    for back in range(reach - 1, 0, -2):
        greet(time + back < times, time + back, own)
        greet(time - back >= 0, time - back, own)
        count += (time + back < times).astype(jnp.int32) + (time - back >= 0).astype(jnp.int32)
    for step in range(1, peers):
        pl.semaphore_signal(barrier, inc=1, **at(time, peer(step, 1)))
    pl.semaphore_signal(barrier, inc=1, **at(twin, own))

    for fill in fills:
        fill.wait()
    shifted = jnp.concatenate(
        [jnp.zeros((1, mine), jnp.float32), before_ref[...].astype(jnp.float32)], 0
    )
    old_ref[...] = shifted.reshape(reach, days, mine).astype(jnp.bfloat16)
    for slot in range(1, reach, 2):
        @pl.when(time + slot < reach)
        def _(slot=slot):
            store_ref[0, odd_place(slot)] = old_ref[time + slot]

    @pl.when(jnp.logical_and(even, time < reach))
    def _():
        store_ref[0, even_place(0)] = old_ref[time]

    sum_ref[...] = jnp.zeros_like(sum_ref)
    lin_ref[...] = jnp.zeros_like(lin_ref)

    pl.semaphore_wait(barrier, count)

    def far(back, place, to):
        return pltpu.make_async_remote_copy(
            src_ref=store_ref.at[0, odd_place(reach)],
            dst_ref=store_ref.at[0, place],
            send_sem=send_far.at[back % reach // 2],
            recv_sem=got_far.at[back % reach // 2],
            **at(to, own),
        )

    @pl.when(forward)
    def _():
        far(reach, even_place(0), time + reach).start()

    for back in range(reach - 1, 0, -2):
        @pl.when(time + back < times)
        def _(back=back):
            far(back, odd_place(reach - back), time + back).start()

    for back in range(2, reach, 2):
        @pl.when(time - back >= 0)
        def _(back=back):
            far(back, odd_place(reach - back), time).wait_recv()

    def across(step, to):
        half = pl.ds(0, 9)
        return pltpu.make_async_remote_copy(
            src_ref=store_ref.at[0, half],
            dst_ref=store_ref.at[step, half],
            send_sem=send_peer.at[step],
            recv_sem=got_peer.at[step],
            **at(time, to),
        )

    def across_edge(step, to):
        return pltpu.make_async_remote_copy(
            src_ref=store_ref.at[0, even_place(0)],
            dst_ref=store_ref.at[step, even_place(0)],
            send_sem=send_edge.at[step],
            recv_sem=got_edge.at[step],
            **at(time, to),
        )

    def over(step, low):
        size = 7 + low
        return pltpu.make_async_remote_copy(
            src_ref=store_ref.at[step, pl.ds(1, size)],
            dst_ref=store_ref.at[step, pl.ds(10 - low, size)],
            send_sem=send_twin.at[step],
            recv_sem=got_twin.at[step],
            **at(twin, own),
        )

    def hand_over(step):
        @pl.when(even)
        def _():
            over(step, 1).start()

        @pl.when(odd)
        def _():
            over(step, 0).start()

    def whole(step, edge):
        @pl.when(even)
        def _():
            over(step, 0).wait_recv()
            if edge:
                across_edge(step, own).wait_recv()

        @pl.when(odd)
        def _():
            over(step, 1).wait_recv()

    def pass_on(step):
        across(step, own).wait_recv()
        hand_over(step)

    hand_over(0)
    for step in range(1, peers):
        across(step, peer(step, 1)).start()

    @pl.when(backward)
    def _():
        far(reach, even_place(0), time).wait_recv()

    @pl.when(even)
    def _():
        for step in range(1, peers):
            across_edge(step, peer(step, 1)).start()

    whole(0, False)

    for start in range(0, mine, TILE):
        x = window(store_ref, 0, pl.ds(start, TILE))
        middle, middle_sq = totals(x)
        for day in range(days):
            center, inverse = day_moments(x, middle, middle_sq, day)
            w = day_values(x, center, inverse * (1.0 / (WIN * shrink_level)), day)
            row_ref[day, :, start : start + TILE] = w
            high = w.astype(jnp.bfloat16).astype(jnp.float32)
            both = jnp.concatenate([high, w - high], 0)
            for sub in range(0, TILE, 128):
                turned = both[:, sub : sub + 128].T.astype(jnp.bfloat16)
                lhs_ref[day, start + sub : start + sub + 128, :128] = turned
                lhs_ref[day, start + sub : start + sub + 128, 128:] = turned

    per_block = mine // TILE
    pairs = per_block // 2
    strips = mine // STRIP
    block_steps = days * pairs * strips

    def prepare(block, parity, piece):
        tile, day = divmod(piece, days)
        cols = pl.ds(tile * TILE, TILE)
        if day == 0:
            x = window(store_ref, block, cols)
            x_ref[...] = x
            middle, middle_sq = totals(x)
            tot_ref[:8] = middle
            tot_ref[8:] = middle_sq
        x, middle, middle_sq = x_ref[...], tot_ref[:8], tot_ref[8:]
        s = store_ref[block, 0, :, cols].astype(jnp.float32)[day : day + 1]
        center, inverse = day_moments(x, middle, middle_sq, day)
        v = day_values(x, center, inverse * s, day)
        lin_ref[day] += v[:, :128] + v[:, 128:]
        high, low = halves(v)
        high_ref[parity, day, tile] = high
        low_ref[parity, day, tile] = low
        bound_ref[parity, day, tile] = jnp.broadcast_to(jnp.abs(s), (8, TILE))

    pieces = days * per_block

    def compute(*accs):
        def push(parity, place):
            day, pair = divmod(place, pairs)
            for unit in range(2):
                high = high_ref[parity, day, 2 * pair + unit]
                low = low_ref[parity, day, 2 * pair + unit]
                pltpu.matmul_push_rhs(
                    jnp.concatenate([high, high, low, low], 0),
                    staging_register=place % 2,
                    mxu_index=unit,
                )

        def take(parity, step):
            place, strip = divmod(step, strips)
            day, pair = divmod(place, pairs)
            rows = pl.ds(strip * STRIP, STRIP)
            part = None
            for unit in range(2):
                bound = bound_ref[parity, day, 2 * pair + unit][:1]
                got = pltpu.matmul_pop(accs[unit * strips + strip])
                kept = jnp.minimum(jnp.maximum(got, -bound), bound)
                kept = kept[:, :128] + kept[:, 128:]
                part = kept if part is None else part + kept
            sum_ref[day, rows, :] += part

        def steps(parity, first, last, piece_at=None, final=False, begin=False):
            for step in range(first, last):
                place, strip = divmod(step, strips)
                day = place // pairs
                lhs = lhs_ref[day, strip * STRIP : (strip + 1) * STRIP, :]
                for unit in range(2):
                    pltpu.matmul_acc_lhs(
                        accs[unit * strips + strip],
                        lhs,
                        load_staged_rhs=place % 2 if strip == 0 else None,
                    )
                if step >= LAG:
                    take(parity, step - LAG)
                elif not begin:
                    take(1 - parity, block_steps + step - LAG)
                if piece_at is not None:
                    piece_at(step)
                if strip == 0:
                    if step + strips < block_steps:
                        push(parity, place + 1)
                    elif not final:
                        push(1 - parity, 0)

        for piece in range(pieces):
            prepare(0, 0, piece)
        push(0, 0)
        quarter = block_steps // 4
        steps(0, 0, quarter, begin=True)
        pass_on(1)
        steps(0, quarter, 2 * quarter + quarter // 2)
        pass_on(2)
        steps(0, 2 * quarter + quarter // 2, 3 * quarter)
        whole(1, True)

        def first_pieces(step):
            for piece in range(pieces):
                if 3 * quarter + piece * (quarter // 2) // pieces == step:
                    prepare(1, 1, piece)

        steps(0, 3 * quarter, block_steps, first_pieces)

        def one_block(block, carry):
            parity = lax.rem(block, 2)
            whole(block + 1, True)

            def next_pieces(step):
                for piece in range(pieces):
                    if LAG + piece * (block_steps - strips - LAG) // pieces == step:
                        prepare(block + 1, 1 - parity, piece)

            steps(parity, 0, block_steps // 2, next_pieces)

            @pl.when(block + 2 < peers)
            def _():
                pass_on(block + 2)

            steps(parity, block_steps // 2, block_steps, next_pieces)
            return carry

        lax.fori_loop(1, peers - 1, one_block, 0)
        parity = (peers - 1) % 2
        steps(parity, 0, block_steps, final=True)
        for step in range(block_steps - LAG, block_steps):
            take(parity, step)

        for day in range(days):
            weight = jnp.sum(lin_ref[day], axis=1, keepdims=True)
            line = jnp.sum(row_ref[day] * weight, axis=0, keepdims=True)
            clamped = jnp.concatenate(
                [
                    jnp.sum(sum_ref[day, start : start + 128, :].T, axis=0, keepdims=True)
                    for start in range(0, mine, 128)
                ],
                1,
            )
            out_ref[day : day + 1, :] = (line - clamped) * shrink_level

    pl.run_scoped(
        compute,
        *[pltpu.ACC(unit)((STRIP, TILE), jnp.float32) for unit in range(2) for _ in range(strips)],
    )

    @pl.when(forward)
    def _():
        far(reach, even_place(0), time).wait_send()

    for back in range(2, reach, 2):
        @pl.when(time + back < times)
        def _(back=back):
            far(back, odd_place(reach - back), time).wait_send()

    for step in range(peers):
        if step:
            across(step, own).wait_send()

        @pl.when(even)
        def _(step=step):
            over(step, 1).wait_send()
            if step:
                across_edge(step, own).wait_send()

        @pl.when(odd)
        def _(step=step):
            over(step, 0).wait_send()


def per_device(returns, signal, earlier):
    days, mine = returns.shape
    peers = lax.axis_size("asset")
    tiles = mine // TILE
    place = pl.BlockSpec(memory_space=pl.ANY)
    vmem, dma = pltpu.VMEM, pltpu.SemaphoreType.DMA
    return pl.pallas_call(
        kernel,
        out_shape=jax.ShapeDtypeStruct((days, mine), jnp.float32),
        in_specs=[place] * 3,
        out_specs=pl.BlockSpec(memory_space=pltpu.VMEM),
        scratch_shapes=[
            vmem((peers, BLOCKS + 1, days, mine), jnp.bfloat16),
            vmem((BLOCKS - 1, days, mine), jnp.bfloat16),
            vmem((HIST, mine), jnp.bfloat16),
            vmem((2, days, tiles, DEPTH, TILE), jnp.bfloat16),
            vmem((2, days, tiles, DEPTH, TILE), jnp.bfloat16),
            vmem((2, days, tiles, 8, TILE), jnp.float32),
            vmem((days, mine, TILE), jnp.bfloat16),
            vmem((days, DEPTH, mine), jnp.float32),
            vmem((days, mine, 128), jnp.float32),
            vmem((days, DEPTH, 128), jnp.float32),
            vmem((DEPTH, TILE), jnp.float32),
            vmem((16, TILE), jnp.float32),
            dma((3,)),
        ]
        + [dma((BLOCKS // 2,))] * 2
        + [dma((peers,))] * 6,
        compiler_params=pltpu.CompilerParams(
            collective_id=0, has_side_effects=True, vmem_limit_bytes=48 << 20
        ),
        name="filter_days",
    )(returns, signal, earlier)


def solution(mesh):
    in_specs = (P("tm", "asset"), P("tm", "asset"), P(None, "asset"))
    out_specs = P("tm", "asset")
    return jax.shard_map(
        per_device, mesh=mesh, in_specs=in_specs, out_specs=out_specs, check_vma=False
    )
```

```python
import jax
import jax.numpy as jnp
from jax import lax
from jax.experimental import pallas as pl
from jax.experimental.pallas import tpu as pltpu
from jax.sharding import PartitionSpec as P

WIN = 60
HIST = 59
DEPTH = 64
TILE = 256
STRIP = 128
LAG = 4
BLOCKS = 16

var_floor = 0.05
shrink_level = 0.1


def totals(x):
    middle = middle_sq = None
    for at in range(0, DEPTH, 8):
        if at in (24, 32):
            continue
        part = x[at : at + 8]
        middle = part if middle is None else middle + part
        middle_sq = part * part if middle_sq is None else middle_sq + part * part
    return middle, middle_sq


def day_edges(x, day):
    row = lax.broadcasted_iota(jnp.int32, (8, x.shape[1]), 0)
    newest = jnp.where(row <= day + 4, x[24:32], 0.0)
    oldest = jnp.where(row >= day + 1, x[32:40], 0.0)
    return newest, oldest


def day_moments(x, middle, middle_sq, day):
    newest, oldest = day_edges(x, day)
    total = jnp.sum(middle + newest + oldest, axis=0, keepdims=True)
    total_sq = jnp.sum(middle_sq + newest * newest + oldest * oldest, axis=0, keepdims=True)
    center = total * (1.0 / WIN)
    spread = total_sq * (1.0 / WIN) - center * center
    return center, lax.rsqrt(jnp.maximum(spread, var_floor))


def day_values(x, center, factor, day):
    scaled = (x - center) * factor
    newest, oldest = day_edges(scaled, day)
    return jnp.concatenate([scaled[:24], newest, oldest, scaled[40:]], 0)


def halves(x):
    high = x.astype(jnp.bfloat16)
    low = (x - high.astype(jnp.float32)).astype(jnp.bfloat16)
    return high, low


def odd_place(slot):
    return 1 + slot // 2


def even_place(slot):
    return 9 + slot // 2


def window(store_ref, block, cols):
    x = store_ref[block, 1:, :, cols].astype(jnp.float32)
    return x.reshape(DEPTH, TILE)


def kernel(
    returns_ref, signal_ref, earlier_ref, out_ref,
    store_ref, old_ref, before_ref, high_ref, low_ref, bound_ref, lhs_ref, row_ref, sum_ref, lin_ref, x_ref, tot_ref,
    fill_sem, send_far, got_far, send_peer, got_peer, send_edge, got_edge, send_twin, got_twin,
):
    days, mine = out_ref.shape
    time, own = lax.axis_index("tm"), lax.axis_index("asset")
    times, peers = lax.axis_size("tm"), lax.axis_size("asset")
    core = lax.rem(time, 2)
    twin = time + 1 - 2 * core
    even, odd = core == 0, core == 1
    reach = BLOCKS - 1
    column, side = own // 2, lax.rem(own, 2)

    def at(t, a):
        return dict(device_id=(t, a), device_id_type=pl.DeviceIdType.MESH)

    def peer(step, sign):
        along = (0, 0, 1, 3, 2, 1, 3, 2)[step]
        other = (0, 1, 0, 0, 0, 1, 1, 1)[step]
        flipped = 1 - side if other else side
        return 2 * lax.rem(column + (along if sign > 0 else peers // 2 - along), peers // 2) + flipped

    fills = [
        pltpu.make_async_copy(returns_ref, store_ref.at[0, odd_place(reach)], fill_sem.at[0]),
        pltpu.make_async_copy(signal_ref, store_ref.at[0, 0], fill_sem.at[1]),
        pltpu.make_async_copy(earlier_ref, before_ref, fill_sem.at[2]),
    ]
    for fill in fills:
        fill.start()

    barrier = pltpu.get_barrier_semaphore()

    def greet(valid, t, a):
        @pl.when(valid)
        def _():
            pl.semaphore_signal(barrier, inc=1, **at(t, a))

    count = peers
    forward = jnp.logical_and(odd, time + reach < times)
    backward = jnp.logical_and(even, time - reach >= 0)
    greet(forward, time + reach, own)
    greet(backward, time - reach, own)
    count += forward.astype(jnp.int32) + backward.astype(jnp.int32)
    for back in range(reach - 1, 0, -2):
        greet(time + back < times, time + back, own)
        greet(time - back >= 0, time - back, own)
        count += (time + back < times).astype(jnp.int32) + (time - back >= 0).astype(jnp.int32)
    for step in range(1, peers):
        pl.semaphore_signal(barrier, inc=1, **at(time, peer(step, 1)))
    pl.semaphore_signal(barrier, inc=1, **at(twin, own))

    for fill in fills:
        fill.wait()
    shifted = jnp.concatenate(
        [jnp.zeros((1, mine), jnp.float32), before_ref[...].astype(jnp.float32)], 0
    )
    old_ref[...] = shifted.reshape(reach, days, mine).astype(jnp.bfloat16)
    for slot in range(1, reach, 2):
        @pl.when(time + slot < reach)
        def _(slot=slot):
            store_ref[0, odd_place(slot)] = old_ref[time + slot]

    @pl.when(jnp.logical_and(even, time < reach))
    def _():
        store_ref[0, even_place(0)] = old_ref[time]

    sum_ref[...] = jnp.zeros_like(sum_ref)
    lin_ref[...] = jnp.zeros_like(lin_ref)

    pl.semaphore_wait(barrier, count)

    def far(back, place, to):
        return pltpu.make_async_remote_copy(
            src_ref=store_ref.at[0, odd_place(reach)],
            dst_ref=store_ref.at[0, place],
            send_sem=send_far.at[back % reach // 2],
            recv_sem=got_far.at[back % reach // 2],
            **at(to, own),
        )

    @pl.when(forward)
    def _():
        far(reach, even_place(0), time + reach).start()

    for back in range(reach - 1, 0, -2):
        @pl.when(time + back < times)
        def _(back=back):
            far(back, odd_place(reach - back), time + back).start()

    for back in range(2, reach, 2):
        @pl.when(time - back >= 0)
        def _(back=back):
            far(back, odd_place(reach - back), time).wait_recv()

    def across(step, to):
        half = pl.ds(0, 9)
        return pltpu.make_async_remote_copy(
            src_ref=store_ref.at[0, half],
            dst_ref=store_ref.at[step, half],
            send_sem=send_peer.at[step],
            recv_sem=got_peer.at[step],
            **at(time, to),
        )

    def across_edge(step, to):
        return pltpu.make_async_remote_copy(
            src_ref=store_ref.at[0, even_place(0)],
            dst_ref=store_ref.at[step, even_place(0)],
            send_sem=send_edge.at[step],
            recv_sem=got_edge.at[step],
            **at(time, to),
        )

    def over(step, low):
        size = 7 + low
        return pltpu.make_async_remote_copy(
            src_ref=store_ref.at[step, pl.ds(1, size)],
            dst_ref=store_ref.at[step, pl.ds(10 - low, size)],
            send_sem=send_twin.at[step],
            recv_sem=got_twin.at[step],
            **at(twin, own),
        )

    def hand_over(step):
        @pl.when(even)
        def _():
            over(step, 1).start()

        @pl.when(odd)
        def _():
            over(step, 0).start()

    def whole(step, edge):
        @pl.when(even)
        def _():
            over(step, 0).wait_recv()
            if edge:
                across_edge(step, own).wait_recv()

        @pl.when(odd)
        def _():
            over(step, 1).wait_recv()

    def pass_on(step):
        across(step, own).wait_recv()
        hand_over(step)

    hand_over(0)
    def send_window(first, last):
        for step in range(first, last):
            across(step, peer(step, 1)).start()

        @pl.when(even)
        def _():
            for step in range(first, last):
                across_edge(step, peer(step, 1)).start()

    nearest = peers // 2

    @pl.when(backward)
    def _():
        far(reach, even_place(0), time).wait_recv()

    send_window(1, nearest)

    whole(0, False)

    for start in range(0, mine, TILE):
        x = window(store_ref, 0, pl.ds(start, TILE))
        middle, middle_sq = totals(x)
        for day in range(days):
            center, inverse = day_moments(x, middle, middle_sq, day)
            w = day_values(x, center, inverse * (1.0 / (WIN * shrink_level)), day)
            row_ref[day, :, start : start + TILE] = w
            high = w.astype(jnp.bfloat16).astype(jnp.float32)
            both = jnp.concatenate([high, w - high], 0)
            for sub in range(0, TILE, 128):
                turned = both[:, sub : sub + 128].T.astype(jnp.bfloat16)
                lhs_ref[day, start + sub : start + sub + 128, :128] = turned
                lhs_ref[day, start + sub : start + sub + 128, 128:] = turned

    per_block = mine // TILE
    pairs = per_block // 2
    strips = mine // STRIP
    block_steps = days * pairs * strips

    def prepare(block, parity, piece):
        tile, day = divmod(piece, days)
        cols = pl.ds(tile * TILE, TILE)
        if day == 0:
            x = window(store_ref, block, cols)
            x_ref[...] = x
            middle, middle_sq = totals(x)
            tot_ref[:8] = middle
            tot_ref[8:] = middle_sq
        x, middle, middle_sq = x_ref[...], tot_ref[:8], tot_ref[8:]
        s = store_ref[block, 0, :, cols].astype(jnp.float32)[day : day + 1]
        center, inverse = day_moments(x, middle, middle_sq, day)
        v = day_values(x, center, inverse * s, day)
        lin_ref[day] += v[:, :128] + v[:, 128:]
        high, low = halves(v)
        high_ref[parity, day, tile] = high
        low_ref[parity, day, tile] = low
        bound_ref[parity, day, tile] = jnp.broadcast_to(jnp.abs(s), (8, TILE))

    pieces = days * per_block

    def compute(*accs):
        def push(parity, place):
            day, pair = divmod(place, pairs)
            for unit in range(2):
                high = high_ref[parity, day, 2 * pair + unit]
                low = low_ref[parity, day, 2 * pair + unit]
                pltpu.matmul_push_rhs(
                    jnp.concatenate([high, high, low, low], 0),
                    staging_register=place % 2,
                    mxu_index=unit,
                )

        def take(parity, step):
            place, strip = divmod(step, strips)
            day, pair = divmod(place, pairs)
            rows = pl.ds(strip * STRIP, STRIP)
            part = None
            for unit in range(2):
                bound = bound_ref[parity, day, 2 * pair + unit][:1]
                got = pltpu.matmul_pop(accs[unit * strips + strip])
                kept = jnp.minimum(jnp.maximum(got, -bound), bound)
                kept = kept[:, :128] + kept[:, 128:]
                part = kept if part is None else part + kept
            sum_ref[day, rows, :] += part

        def steps(parity, first, last, piece_at=None, final=False, begin=False):
            for step in range(first, last):
                place, strip = divmod(step, strips)
                day = place // pairs
                lhs = lhs_ref[day, strip * STRIP : (strip + 1) * STRIP, :]
                for unit in range(2):
                    pltpu.matmul_acc_lhs(
                        accs[unit * strips + strip],
                        lhs,
                        load_staged_rhs=place % 2 if strip == 0 else None,
                    )
                if step >= LAG:
                    take(parity, step - LAG)
                elif not begin:
                    take(1 - parity, block_steps + step - LAG)
                if piece_at is not None:
                    piece_at(step)
                if strip == 0:
                    if step + strips < block_steps:
                        push(parity, place + 1)
                    elif not final:
                        push(1 - parity, 0)

        for piece in range(pieces):
            prepare(0, 0, piece)
        push(0, 0)
        quarter = block_steps // 4
        steps(0, 0, quarter, begin=True)
        pass_on(1)
        send_window(nearest, peers)
        steps(0, quarter, 2 * quarter + quarter // 2)
        pass_on(2)
        steps(0, 2 * quarter + quarter // 2, 3 * quarter)
        whole(1, True)

        def first_pieces(step):
            for piece in range(pieces):
                if 3 * quarter + piece * (quarter // 2) // pieces == step:
                    prepare(1, 1, piece)

        steps(0, 3 * quarter, block_steps, first_pieces)

        def one_block(block, carry):
            parity = lax.rem(block, 2)
            whole(block + 1, True)

            def next_pieces(step):
                for piece in range(pieces):
                    if LAG + piece * (block_steps - strips - LAG) // pieces == step:
                        prepare(block + 1, 1 - parity, piece)

            steps(parity, 0, block_steps // 2, next_pieces)

            @pl.when(block + 2 < peers)
            def _():
                pass_on(block + 2)

            steps(parity, block_steps // 2, block_steps, next_pieces)
            return carry

        lax.fori_loop(1, peers - 1, one_block, 0)
        parity = (peers - 1) % 2
        steps(parity, 0, block_steps, final=True)
        for step in range(block_steps - LAG, block_steps):
            take(parity, step)

        for day in range(days):
            weight = jnp.sum(lin_ref[day], axis=1, keepdims=True)
            line = jnp.sum(row_ref[day] * weight, axis=0, keepdims=True)
            clamped = jnp.concatenate(
                [
                    jnp.sum(sum_ref[day, start : start + 128, :].T, axis=0, keepdims=True)
                    for start in range(0, mine, 128)
                ],
                1,
            )
            out_ref[day : day + 1, :] = (line - clamped) * shrink_level

    pl.run_scoped(
        compute,
        *[pltpu.ACC(unit)((STRIP, TILE), jnp.float32) for unit in range(2) for _ in range(strips)],
    )

    @pl.when(forward)
    def _():
        far(reach, even_place(0), time).wait_send()

    for back in range(2, reach, 2):
        @pl.when(time + back < times)
        def _(back=back):
            far(back, odd_place(reach - back), time).wait_send()

    for step in range(peers):
        if step:
            across(step, own).wait_send()

        @pl.when(even)
        def _(step=step):
            over(step, 1).wait_send()
            if step:
                across_edge(step, own).wait_send()

        @pl.when(odd)
        def _(step=step):
            over(step, 0).wait_send()


def per_device(returns, signal, earlier):
    days, mine = returns.shape
    peers = lax.axis_size("asset")
    tiles = mine // TILE
    place = pl.BlockSpec(memory_space=pl.ANY)
    vmem, dma = pltpu.VMEM, pltpu.SemaphoreType.DMA
    return pl.pallas_call(
        kernel,
        out_shape=jax.ShapeDtypeStruct((days, mine), jnp.float32),
        in_specs=[place] * 3,
        out_specs=pl.BlockSpec(memory_space=pltpu.VMEM),
        scratch_shapes=[
            vmem((peers, BLOCKS + 1, days, mine), jnp.bfloat16),
            vmem((BLOCKS - 1, days, mine), jnp.bfloat16),
            vmem((HIST, mine), jnp.bfloat16),
            vmem((2, days, tiles, DEPTH, TILE), jnp.bfloat16),
            vmem((2, days, tiles, DEPTH, TILE), jnp.bfloat16),
            vmem((2, days, tiles, 8, TILE), jnp.float32),
            vmem((days, mine, TILE), jnp.bfloat16),
            vmem((days, DEPTH, mine), jnp.float32),
            vmem((days, mine, 128), jnp.float32),
            vmem((days, DEPTH, 128), jnp.float32),
            vmem((DEPTH, TILE), jnp.float32),
            vmem((16, TILE), jnp.float32),
            dma((3,)),
        ]
        + [dma((BLOCKS // 2,))] * 2
        + [dma((peers,))] * 6,
        compiler_params=pltpu.CompilerParams(
            collective_id=0, has_side_effects=True, vmem_limit_bytes=48 << 20
        ),
        name="filter_days",
    )(*(pltpu.with_memory_space_constraint(x, pltpu.HBM) for x in (returns, signal, earlier)))


def solution(mesh):
    in_specs = (P("tm", "asset"), P("tm", "asset"), P(None, "asset"))
    out_specs = P("tm", "asset")
    return jax.shard_map(
        per_device, mesh=mesh, in_specs=in_specs, out_specs=out_specs, check_vma=False
    )
```

```python
import jax
import jax.numpy as jnp
from jax import lax
from jax.experimental import pallas as pl
from jax.experimental.pallas import tpu as pltpu
from jax.sharding import PartitionSpec as P

WIN = 60
HIST = 59
DEPTH = 64
TILE = 256
STRIP = 128
LAG = 0
SPARE = 8
BLOCKS = 16

var_floor = 0.05
shrink_level = 0.1


def totals(x):
    middle = middle_sq = None
    for at in range(0, DEPTH, 8):
        if at in (24, 32):
            continue
        part = x[at : at + 8]
        middle = part if middle is None else middle + part
        middle_sq = part * part if middle_sq is None else middle_sq + part * part
    return middle, middle_sq


def day_edges(x, day):
    row = lax.broadcasted_iota(jnp.int32, (8, x.shape[1]), 0)
    newest = jnp.where(row <= day + 4, x[24:32], 0.0)
    oldest = jnp.where(row >= day + 1, x[32:40], 0.0)
    return newest, oldest


def day_moments(x, middle, middle_sq, day):
    newest, oldest = day_edges(x, day)
    total = jnp.sum(middle + newest + oldest, axis=0, keepdims=True)
    total_sq = jnp.sum(middle_sq + newest * newest + oldest * oldest, axis=0, keepdims=True)
    center = total * (1.0 / WIN)
    spread = total_sq * (1.0 / WIN) - center * center
    return center, lax.rsqrt(jnp.maximum(spread, var_floor))


def day_values(x, center, factor, day):
    scaled = (x - center) * factor
    newest, oldest = day_edges(scaled, day)
    return jnp.concatenate([scaled[:24], newest, oldest, scaled[40:]], 0)


def halves(x):
    high = x.astype(jnp.bfloat16)
    low = (x - high.astype(jnp.float32)).astype(jnp.bfloat16)
    return high, low


def odd_place(slot):
    return 1 + slot // 2


def even_place(slot):
    return 9 + slot // 2


def window(store_ref, block, cols):
    x = store_ref[block, 1 : 1 + BLOCKS, :, cols].astype(jnp.float32)
    return x.reshape(DEPTH, TILE)


def kernel(
    returns_ref, signal_ref, earlier_ref, out_ref,
    store_ref, old_ref, before_ref, high_ref, low_ref, bound_ref, lhs_ref, row_ref, sum_ref, lin_ref, x_ref, tot_ref,
    fill_sem, send_far, got_far, send_peer, got_peer, send_edge, got_edge, send_twin, got_twin,
):
    days, mine = out_ref.shape
    time, own = lax.axis_index("tm"), lax.axis_index("asset")
    times, peers = lax.axis_size("tm"), lax.axis_size("asset")
    core = lax.rem(time, 2)
    twin = time + 1 - 2 * core
    even, odd = core == 0, core == 1
    reach = BLOCKS - 1
    column, side = own // 2, lax.rem(own, 2)

    def at(t, a):
        return dict(device_id=(t, a), device_id_type=pl.DeviceIdType.MESH)

    def peer(step, sign):
        along = (0, 0, 1, 3, 2, 1, 3, 2)[step]
        other = (0, 1, 0, 0, 0, 1, 1, 1)[step]
        flipped = 1 - side if other else side
        return 2 * lax.rem(column + (along if sign > 0 else peers // 2 - along), peers // 2) + flipped

    fills = [
        pltpu.make_async_copy(returns_ref, store_ref.at[0, odd_place(reach)], fill_sem.at[0]),
        pltpu.make_async_copy(signal_ref, store_ref.at[0, 0], fill_sem.at[1]),
        pltpu.make_async_copy(earlier_ref, before_ref, fill_sem.at[2]),
    ]
    for fill in fills:
        fill.start()

    barrier = pltpu.get_barrier_semaphore()

    def greet(valid, t, a):
        @pl.when(valid)
        def _():
            pl.semaphore_signal(barrier, inc=1, **at(t, a))

    count = peers
    forward = jnp.logical_and(odd, time + reach < times)
    backward = jnp.logical_and(even, time - reach >= 0)
    greet(forward, time + reach, own)
    greet(backward, time - reach, own)
    count += forward.astype(jnp.int32) + backward.astype(jnp.int32)
    for back in range(reach - 1, 0, -2):
        greet(time + back < times, time + back, own)
        greet(time - back >= 0, time - back, own)
        count += (time + back < times).astype(jnp.int32) + (time - back >= 0).astype(jnp.int32)
    for step in range(1, peers):
        pl.semaphore_signal(barrier, inc=1, **at(time, peer(step, 1)))
    pl.semaphore_signal(barrier, inc=1, **at(twin, own))

    for fill in fills:
        fill.wait()
    shifted = jnp.concatenate(
        [jnp.zeros((1, mine), jnp.float32), before_ref[...].astype(jnp.float32)], 0
    )
    old_ref[...] = shifted.reshape(reach, days, mine).astype(jnp.bfloat16)
    for slot in range(1, reach, 2):
        @pl.when(time + slot < reach)
        def _(slot=slot):
            store_ref[0, odd_place(slot)] = old_ref[time + slot]

    @pl.when(jnp.logical_and(even, time < reach))
    def _():
        store_ref[0, even_place(0)] = old_ref[time]

    sum_ref[...] = jnp.zeros_like(sum_ref)
    lin_ref[...] = jnp.zeros_like(lin_ref)

    pl.semaphore_wait(barrier, count)

    def far(back, place, to):
        return pltpu.make_async_remote_copy(
            src_ref=store_ref.at[0, odd_place(reach)],
            dst_ref=store_ref.at[0, place],
            send_sem=send_far.at[back % reach // 2],
            recv_sem=got_far.at[back % reach // 2],
            **at(to, own),
        )

    @pl.when(forward)
    def _():
        far(reach, even_place(0), time + reach).start()

    for back in range(reach - 1, 0, -2):
        @pl.when(time + back < times)
        def _(back=back):
            far(back, odd_place(reach - back), time + back).start()

    for back in range(2, reach, 2):
        @pl.when(time - back >= 0)
        def _(back=back):
            far(back, odd_place(reach - back), time).wait_recv()

    def across(step, to):
        half = pl.ds(0, 9)
        return pltpu.make_async_remote_copy(
            src_ref=store_ref.at[0, half],
            dst_ref=store_ref.at[step, half],
            send_sem=send_peer.at[step],
            recv_sem=got_peer.at[step],
            **at(time, to),
        )

    def across_edge(step, to):
        return pltpu.make_async_remote_copy(
            src_ref=store_ref.at[0, even_place(0) - core],
            dst_ref=store_ref.at[step, even_place(0) + core * SPARE],
            send_sem=send_edge.at[step],
            recv_sem=got_edge.at[step],
            **at(time, to),
        )

    def over(step):
        return pltpu.make_async_remote_copy(
            src_ref=store_ref.at[step, pl.ds(1, 8)],
            dst_ref=store_ref.at[step, pl.ds(9 + core, 8)],
            send_sem=send_twin.at[step],
            recv_sem=got_twin.at[step],
            **at(twin, own),
        )

    def whole(step, edge):
        over(step).wait_recv()
        if edge:
            across_edge(step, own).wait_recv()

    def pass_on(step):
        across(step, own).wait_recv()
        over(step).start()

    over(0).start()
    def send_window(first, last):
        for step in range(first, last):
            across(step, peer(step, 1)).start()
            across_edge(step, peer(step, 1)).start()

    nearest = peers // 2

    @pl.when(backward)
    def _():
        far(reach, even_place(0), time).wait_recv()

    send_window(1, nearest)

    whole(0, False)

    per_block = mine // TILE
    pairs = per_block // 2
    strips = mine // STRIP
    block_steps = days * pairs * strips

    def prepare(block, parity, piece, both_sides=False):
        tile, day = divmod(piece, days)
        cols = pl.ds(tile * TILE, TILE)
        if day == 0:
            x = window(store_ref, block, cols)
            x_ref[...] = x
            middle, middle_sq = totals(x)
            tot_ref[:8] = middle
            tot_ref[8:] = middle_sq
        x, middle, middle_sq = x_ref[...], tot_ref[:8], tot_ref[8:]
        s = store_ref[block, 0, :, cols].astype(jnp.float32)[day : day + 1]
        center, inverse = day_moments(x, middle, middle_sq, day)
        v = day_values(x, center, inverse * s, day)
        lin_ref[day] += v[:, :128] + v[:, 128:]
        high, low = halves(v)
        high_ref[parity, day, tile] = high
        low_ref[parity, day, tile] = low
        bound_ref[parity, day, tile] = jnp.broadcast_to(jnp.abs(s), (8, TILE))
        if both_sides:
            start = tile * TILE
            w = day_values(x, center, inverse * (1.0 / (WIN * shrink_level)), day)
            row_ref[day, :, start : start + TILE] = w
            high = w.astype(jnp.bfloat16).astype(jnp.float32)
            both = jnp.concatenate([high, w - high], 0)
            for sub in range(0, TILE, 128):
                turned = both[:, sub : sub + 128].T.astype(jnp.bfloat16)
                lhs_ref[day, start + sub : start + sub + 128, :128] = turned
                lhs_ref[day, start + sub : start + sub + 128, 128:] = turned

    pieces = days * per_block

    def compute(*accs):
        def push(parity, place):
            day, pair = divmod(place, pairs)
            for unit in range(2):
                high = high_ref[parity, day, 2 * pair + unit]
                low = low_ref[parity, day, 2 * pair + unit]
                pltpu.matmul_push_rhs(
                    jnp.concatenate([high, high, low, low], 0),
                    staging_register=place % 2,
                    mxu_index=unit,
                )

        def take(parity, step):
            place, strip = divmod(step, strips)
            day, pair = divmod(place, pairs)
            rows = pl.ds(strip * STRIP, STRIP)
            part = None
            for unit in range(2):
                bound = bound_ref[parity, day, 2 * pair + unit][:1]
                got = pltpu.matmul_pop(accs[unit * strips + strip])
                kept = jnp.minimum(jnp.maximum(got, -bound), bound)
                kept = kept[:, :128] + kept[:, 128:]
                part = kept if part is None else part + kept
            sum_ref[day, rows, :] += part

        def steps(parity, first, last, piece_at=None, final=False, begin=False):
            for step in range(first, last):
                place, strip = divmod(step, strips)
                day = place // pairs
                lhs = lhs_ref[day, strip * STRIP : (strip + 1) * STRIP, :]
                for unit in range(2):
                    pltpu.matmul_acc_lhs(
                        accs[unit * strips + strip],
                        lhs,
                        load_staged_rhs=place % 2 if strip == 0 else None,
                    )
                if step >= LAG:
                    take(parity, step - LAG)
                elif not begin:
                    take(1 - parity, block_steps + step - LAG)
                if piece_at is not None:
                    piece_at(step)
                if strip == 0:
                    if step + strips < block_steps:
                        push(parity, place + 1)
                    elif not final:
                        push(1 - parity, 0)

        for piece in range(pieces):
            prepare(0, 0, piece, True)
        push(0, 0)
        quarter = block_steps // 4
        steps(0, 0, quarter + 4, begin=True)
        pass_on(1)
        send_window(nearest, peers)
        steps(0, quarter + 4, 3 * quarter)
        pass_on(2)
        whole(1, True)

        def first_pieces(step):
            for piece in range(pieces):
                if 3 * quarter + piece * (quarter // 2) // pieces == step:
                    prepare(1, 1, piece)

        steps(0, 3 * quarter, block_steps, first_pieces)

        def one_block(block, carry):
            parity = lax.rem(block, 2)
            whole(block + 1, True)

            @pl.when(block + 2 < peers)
            def _():
                pass_on(block + 2)

            def next_pieces(step):
                for piece in range(pieces):
                    if 4 + piece * (block_steps - strips - 4) // pieces == step:
                        prepare(block + 1, 1 - parity, piece)

            steps(parity, 0, block_steps, next_pieces)
            return carry

        lax.fori_loop(1, peers - 1, one_block, 0)
        parity = (peers - 1) % 2
        steps(parity, 0, block_steps, final=True)
        for step in range(block_steps - LAG, block_steps):
            take(parity, step)

        for day in range(days):
            weight = jnp.sum(lin_ref[day], axis=1, keepdims=True)
            line = jnp.sum(row_ref[day] * weight, axis=0, keepdims=True)
            clamped = jnp.concatenate(
                [
                    jnp.sum(sum_ref[day, start : start + 128, :].T, axis=0, keepdims=True)
                    for start in range(0, mine, 128)
                ],
                1,
            )
            out_ref[day : day + 1, :] = (line - clamped) * shrink_level

    pl.run_scoped(
        compute,
        *[pltpu.ACC(unit)((STRIP, TILE), jnp.float32) for unit in range(2) for _ in range(strips)],
    )

    @pl.when(forward)
    def _():
        far(reach, even_place(0), time).wait_send()

    for back in range(2, reach, 2):
        @pl.when(time + back < times)
        def _(back=back):
            far(back, odd_place(reach - back), time).wait_send()

    for step in range(peers):
        over(step).wait_send()
        if step:
            across(step, own).wait_send()
            across_edge(step, own).wait_send()


def per_device(returns, signal, earlier):
    days, mine = returns.shape
    peers = lax.axis_size("asset")
    tiles = mine // TILE
    place = pl.BlockSpec(memory_space=pl.ANY)
    vmem, dma = pltpu.VMEM, pltpu.SemaphoreType.DMA
    return pl.pallas_call(
        kernel,
        out_shape=jax.ShapeDtypeStruct((days, mine), jnp.float32),
        in_specs=[place] * 3,
        out_specs=pl.BlockSpec(memory_space=pltpu.VMEM),
        scratch_shapes=[
            vmem((peers, BLOCKS + 2, days, mine), jnp.bfloat16),
            vmem((BLOCKS - 1, days, mine), jnp.bfloat16),
            vmem((HIST, mine), jnp.bfloat16),
            vmem((2, days, tiles, DEPTH, TILE), jnp.bfloat16),
            vmem((2, days, tiles, DEPTH, TILE), jnp.bfloat16),
            vmem((2, days, tiles, 8, TILE), jnp.float32),
            vmem((days, mine, TILE), jnp.bfloat16),
            vmem((days, DEPTH, mine), jnp.float32),
            vmem((days, mine, 128), jnp.float32),
            vmem((days, DEPTH, 128), jnp.float32),
            vmem((DEPTH, TILE), jnp.float32),
            vmem((16, TILE), jnp.float32),
            dma((3,)),
        ]
        + [dma((BLOCKS // 2,))] * 2
        + [dma((peers,))] * 6,
        compiler_params=pltpu.CompilerParams(
            collective_id=0, has_side_effects=True, vmem_limit_bytes=48 << 20
        ),
        name="filter_days",
    )(*(pltpu.with_memory_space_constraint(x, pltpu.HBM) for x in (returns, signal, earlier)))


def solution(mesh):
    in_specs = (P("tm", "asset"), P("tm", "asset"), P(None, "asset"))
    out_specs = P("tm", "asset")
    return jax.shard_map(
        per_device, mesh=mesh, in_specs=in_specs, out_specs=out_specs, check_vma=False
    )
```

```python
import jax
import jax.numpy as jnp
from jax import lax
from jax.experimental import pallas as pl
from jax.experimental.pallas import tpu as pltpu
from jax.sharding import PartitionSpec as P

WIN = 60
HIST = 59
DEPTH = 64
TILE = 256
STRIP = 128
LAG = 0
SPARE = 8
FIRST_WAIT = 28
SECOND_WAIT = 52
OWN_AT = (0, 4, 8, 12)
PIECE_AT = 4
PIECE_SPAN = 60
BLOCKS = 16

var_floor = 0.05
shrink_level = 0.1


def totals(x):
    middle = middle_sq = None
    for at in range(0, DEPTH, 8):
        if at in (24, 32):
            continue
        part = x[at : at + 8]
        middle = part if middle is None else middle + part
        middle_sq = part * part if middle_sq is None else middle_sq + part * part
    return middle, middle_sq


def day_edges(x, day):
    row = lax.broadcasted_iota(jnp.int32, (8, x.shape[1]), 0)
    newest = jnp.where(row <= day + 4, x[24:32], 0.0)
    oldest = jnp.where(row >= day + 1, x[32:40], 0.0)
    return newest, oldest


def day_moments(x, middle, middle_sq, day):
    newest, oldest = day_edges(x, day)
    total = jnp.sum(middle + newest + oldest, axis=0, keepdims=True)
    total_sq = jnp.sum(middle_sq + newest * newest + oldest * oldest, axis=0, keepdims=True)
    center = total * (1.0 / WIN)
    spread = total_sq * (1.0 / WIN) - center * center
    return center, lax.rsqrt(jnp.maximum(spread, var_floor))


def day_values(x, center, factor, day):
    scaled = (x - center) * factor
    newest, oldest = day_edges(scaled, day)
    return jnp.concatenate([scaled[:24], newest, oldest, scaled[40:]], 0)


def halves(x):
    high = x.astype(jnp.bfloat16)
    low = (x - high.astype(jnp.float32)).astype(jnp.bfloat16)
    return high, low


def odd_place(slot):
    return 1 + slot // 2


def even_place(slot):
    return 9 + slot // 2


def window(store_ref, block, cols):
    x = store_ref[block, 1 : 1 + BLOCKS, :, cols].astype(jnp.float32)
    return x.reshape(DEPTH, TILE)


def kernel(
    returns_ref, signal_ref, earlier_ref, out_ref,
    store_ref, old_ref, before_ref, high_ref, low_ref, bound_ref, lhs_ref, row_ref, sum_ref, lin_ref, x_ref, tot_ref,
    fill_sem, send_far, got_far, send_peer, got_peer, send_edge, got_edge, send_twin, got_twin,
):
    days, mine = out_ref.shape
    time, own = lax.axis_index("tm"), lax.axis_index("asset")
    times, peers = lax.axis_size("tm"), lax.axis_size("asset")
    core = lax.rem(time, 2)
    twin = time + 1 - 2 * core
    even, odd = core == 0, core == 1
    reach = BLOCKS - 1
    column, side = own // 2, lax.rem(own, 2)

    def at(t, a):
        return dict(device_id=(t, a), device_id_type=pl.DeviceIdType.MESH)

    def peer(step, sign):
        along = (0, 0, 1, 3, 2, 1, 3, 2)[step]
        other = (0, 1, 0, 0, 0, 1, 1, 1)[step]
        flipped = 1 - side if other else side
        return 2 * lax.rem(column + (along if sign > 0 else peers // 2 - along), peers // 2) + flipped

    fills = [
        pltpu.make_async_copy(returns_ref, store_ref.at[0, odd_place(reach)], fill_sem.at[0]),
        pltpu.make_async_copy(signal_ref, store_ref.at[0, 0], fill_sem.at[1]),
        pltpu.make_async_copy(earlier_ref, before_ref, fill_sem.at[2]),
    ]
    for fill in fills:
        fill.start()

    barrier = pltpu.get_barrier_semaphore()

    def greet(valid, t, a):
        @pl.when(valid)
        def _():
            pl.semaphore_signal(barrier, inc=1, **at(t, a))

    count = peers
    forward = jnp.logical_and(odd, time + reach < times)
    backward = jnp.logical_and(even, time - reach >= 0)
    greet(forward, time + reach, own)
    greet(backward, time - reach, own)
    count += forward.astype(jnp.int32) + backward.astype(jnp.int32)
    for back in range(reach - 1, 0, -2):
        greet(time + back < times, time + back, own)
        greet(time - back >= 0, time - back, own)
        count += (time + back < times).astype(jnp.int32) + (time - back >= 0).astype(jnp.int32)
    for step in range(1, peers):
        pl.semaphore_signal(barrier, inc=1, **at(time, peer(step, 1)))
    pl.semaphore_signal(barrier, inc=1, **at(twin, own))

    for fill in fills:
        fill.wait()
    shifted = jnp.concatenate(
        [jnp.zeros((1, mine), jnp.float32), before_ref[...].astype(jnp.float32)], 0
    )
    old_ref[...] = shifted.reshape(reach, days, mine).astype(jnp.bfloat16)
    for slot in range(1, reach, 2):
        @pl.when(time + slot < reach)
        def _(slot=slot):
            store_ref[0, odd_place(slot)] = old_ref[time + slot]

    @pl.when(jnp.logical_and(even, time < reach))
    def _():
        store_ref[0, even_place(0)] = old_ref[time]

    sum_ref[...] = jnp.zeros_like(sum_ref)
    lin_ref[...] = jnp.zeros_like(lin_ref)

    pl.semaphore_wait(barrier, count)

    def far(back, place, to):
        return pltpu.make_async_remote_copy(
            src_ref=store_ref.at[0, odd_place(reach)],
            dst_ref=store_ref.at[0, place],
            send_sem=send_far.at[back % reach // 2],
            recv_sem=got_far.at[back % reach // 2],
            **at(to, own),
        )

    @pl.when(forward)
    def _():
        far(reach, even_place(0), time + reach).start()

    for back in range(reach - 1, 0, -2):
        @pl.when(time + back < times)
        def _(back=back):
            far(back, odd_place(reach - back), time + back).start()

    for back in range(2, reach, 2):
        @pl.when(time - back >= 0)
        def _(back=back):
            far(back, odd_place(reach - back), time).wait_recv()

    def across(step, to):
        half = pl.ds(0, 9)
        return pltpu.make_async_remote_copy(
            src_ref=store_ref.at[0, half],
            dst_ref=store_ref.at[step, half],
            send_sem=send_peer.at[step],
            recv_sem=got_peer.at[step],
            **at(time, to),
        )

    def across_edge(step, to):
        return pltpu.make_async_remote_copy(
            src_ref=store_ref.at[0, even_place(0) - core],
            dst_ref=store_ref.at[step, even_place(0) + core * SPARE],
            send_sem=send_edge.at[step],
            recv_sem=got_edge.at[step],
            **at(time, to),
        )

    def over(step):
        return pltpu.make_async_remote_copy(
            src_ref=store_ref.at[step, pl.ds(1, 8)],
            dst_ref=store_ref.at[step, pl.ds(9 + core, 8)],
            send_sem=send_twin.at[step],
            recv_sem=got_twin.at[step],
            **at(twin, own),
        )

    def whole(step, edge):
        over(step).wait_recv()
        if edge:
            across_edge(step, own).wait_recv()

    def pass_on(step):
        across(step, own).wait_recv()
        over(step).start()

    over(0).start()
    def send_window(first, last):
        for step in range(first, last):
            across(step, peer(step, 1)).start()
            across_edge(step, peer(step, 1)).start()

    nearest = peers // 2

    @pl.when(backward)
    def _():
        far(reach, even_place(0), time).wait_recv()

    send_window(1, nearest)

    whole(0, False)

    per_block = mine // TILE
    pairs = per_block // 2
    strips = mine // STRIP
    block_steps = days * pairs * strips

    def prepare(block, parity, piece, both_sides=False):
        tile, day = divmod(piece, days)
        cols = pl.ds(tile * TILE, TILE)
        if day == 0:
            x = window(store_ref, block, cols)
            x_ref[tile] = x
            middle, middle_sq = totals(x)
            tot_ref[tile, :8] = middle
            tot_ref[tile, 8:] = middle_sq
        x, middle, middle_sq = x_ref[tile], tot_ref[tile, :8], tot_ref[tile, 8:]
        s = store_ref[block, 0, :, cols].astype(jnp.float32)[day : day + 1]
        center, inverse = day_moments(x, middle, middle_sq, day)
        v = day_values(x, center, inverse * s, day)
        lin_ref[day] += v[:, :128] + v[:, 128:]
        high, low = halves(v)
        high_ref[parity, day, tile] = high
        low_ref[parity, day, tile] = low
        bound_ref[parity, day, tile] = jnp.broadcast_to(jnp.abs(s), (8, TILE))
        if both_sides:
            start = tile * TILE
            w = day_values(x, center, inverse * (1.0 / (WIN * shrink_level)), day)
            row_ref[day, :, start : start + TILE] = w
            high = w.astype(jnp.bfloat16).astype(jnp.float32)
            both = jnp.concatenate([high, w - high], 0)
            for sub in range(0, TILE, 128):
                turned = both[:, sub : sub + 128].T.astype(jnp.bfloat16)
                lhs_ref[day, start + sub : start + sub + 128, :128] = turned
                lhs_ref[day, start + sub : start + sub + 128, 128:] = turned

    pieces = days * per_block

    def compute(*accs):
        def push(parity, place):
            day, pair = divmod(place, pairs)
            for unit in range(2):
                high = high_ref[parity, day, 2 * pair + unit]
                low = low_ref[parity, day, 2 * pair + unit]
                pltpu.matmul_push_rhs(
                    jnp.concatenate([high, high, low, low], 0),
                    staging_register=place % 2,
                    mxu_index=unit,
                )

        def take(parity, step):
            place, strip = divmod(step, strips)
            day, pair = divmod(place, pairs)
            rows = pl.ds(strip * STRIP, STRIP)
            part = None
            for unit in range(2):
                bound = bound_ref[parity, day, 2 * pair + unit][:1]
                got = pltpu.matmul_pop(accs[unit * strips + strip])
                kept = jnp.minimum(jnp.maximum(got, -bound), bound)
                kept = kept[:, :128] + kept[:, 128:]
                part = kept if part is None else part + kept
            sum_ref[day, rows, :] += part

        def steps(parity, first, last, piece_at=None, final=False, begin=False):
            for step in range(first, last):
                place, strip = divmod(step, strips)
                day = place // pairs
                lhs = lhs_ref[day, strip * STRIP : (strip + 1) * STRIP, :]
                for unit in range(2):
                    pltpu.matmul_acc_lhs(
                        accs[unit * strips + strip],
                        lhs,
                        load_staged_rhs=place % 2 if strip == 0 else None,
                    )
                if step >= LAG:
                    take(parity, step - LAG)
                elif not begin:
                    take(1 - parity, block_steps + step - LAG)
                if piece_at is not None:
                    piece_at(step)
                if strip == 0:
                    if step + strips < block_steps:
                        push(parity, place + 1)
                    elif not final:
                        push(1 - parity, 0)

        quarter = block_steps // 4
        for tile in range(per_block):
            prepare(0, 0, tile * days, True)

        def own_pieces(step):
            day, within = divmod(step, quarter)
            for tile in range(per_block):
                if day + 1 < days and within == OWN_AT[tile]:
                    prepare(0, 0, tile * days + day + 1, True)

        push(0, 0)
        steps(0, 0, FIRST_WAIT, own_pieces, begin=True)
        pass_on(1)
        send_window(nearest, peers)
        steps(0, FIRST_WAIT, SECOND_WAIT, own_pieces)
        pass_on(2)
        whole(1, True)

        def first_pieces(step):
            for piece in range(pieces):
                if SECOND_WAIT + piece * (block_steps - SECOND_WAIT - 1) // pieces == step:
                    prepare(1, 1, piece)

        steps(0, SECOND_WAIT, block_steps, first_pieces)

        def one_block(block, carry):
            parity = lax.rem(block, 2)
            whole(block + 1, True)

            @pl.when(block + 2 < peers)
            def _():
                pass_on(block + 2)

            def next_pieces(step):
                for piece in range(pieces):
                    if PIECE_AT + piece * PIECE_SPAN // pieces == step:
                        prepare(block + 1, 1 - parity, piece)

            steps(parity, 0, block_steps, next_pieces)
            return carry

        lax.fori_loop(1, peers - 1, one_block, 0)
        parity = (peers - 1) % 2
        steps(parity, 0, block_steps, final=True)
        for step in range(block_steps - LAG, block_steps):
            take(parity, step)

        for day in range(days):
            weight = jnp.sum(lin_ref[day], axis=1, keepdims=True)
            line = jnp.sum(row_ref[day] * weight, axis=0, keepdims=True)
            clamped = jnp.concatenate(
                [
                    jnp.sum(sum_ref[day, start : start + 128, :].T, axis=0, keepdims=True)
                    for start in range(0, mine, 128)
                ],
                1,
            )
            out_ref[day : day + 1, :] = (line - clamped) * shrink_level

    pl.run_scoped(
        compute,
        *[pltpu.ACC(unit)((STRIP, TILE), jnp.float32) for unit in range(2) for _ in range(strips)],
    )

    @pl.when(forward)
    def _():
        far(reach, even_place(0), time).wait_send()

    for back in range(2, reach, 2):
        @pl.when(time + back < times)
        def _(back=back):
            far(back, odd_place(reach - back), time).wait_send()

    for step in range(peers):
        over(step).wait_send()
        if step:
            across(step, own).wait_send()
            across_edge(step, own).wait_send()


def per_device(returns, signal, earlier):
    days, mine = returns.shape
    peers = lax.axis_size("asset")
    tiles = mine // TILE
    place = pl.BlockSpec(memory_space=pl.ANY)
    vmem, dma = pltpu.VMEM, pltpu.SemaphoreType.DMA
    return pl.pallas_call(
        kernel,
        out_shape=jax.ShapeDtypeStruct((days, mine), jnp.float32),
        in_specs=[place] * 3,
        out_specs=pl.BlockSpec(memory_space=pltpu.VMEM),
        scratch_shapes=[
            vmem((peers, BLOCKS + 2, days, mine), jnp.bfloat16),
            vmem((BLOCKS - 1, days, mine), jnp.bfloat16),
            vmem((HIST, mine), jnp.bfloat16),
            vmem((2, days, tiles, DEPTH, TILE), jnp.bfloat16),
            vmem((2, days, tiles, DEPTH, TILE), jnp.bfloat16),
            vmem((2, days, tiles, 8, TILE), jnp.float32),
            vmem((days, mine, TILE), jnp.bfloat16),
            vmem((days, DEPTH, mine), jnp.float32),
            vmem((days, mine, 128), jnp.float32),
            vmem((days, DEPTH, 128), jnp.float32),
            vmem((tiles, DEPTH, TILE), jnp.float32),
            vmem((tiles, 16, TILE), jnp.float32),
            dma((3,)),
        ]
        + [dma((BLOCKS // 2,))] * 2
        + [dma((peers,))] * 6,
        compiler_params=pltpu.CompilerParams(
            collective_id=0, has_side_effects=True, vmem_limit_bytes=48 << 20
        ),
        name="filter_days",
    )(*(pltpu.with_memory_space_constraint(x, pltpu.HBM) for x in (returns, signal, earlier)))


def solution(mesh):
    in_specs = (P("tm", "asset"), P("tm", "asset"), P(None, "asset"))
    out_specs = P("tm", "asset")
    return jax.shard_map(
        per_device, mesh=mesh, in_specs=in_specs, out_specs=out_specs, check_vma=False
    )
```

```python
import jax
import jax.numpy as jnp
from jax import lax
from jax.experimental import pallas as pl
from jax.experimental.pallas import tpu as pltpu
from jax.sharding import PartitionSpec as P

WIN = 60
HIST = 59
DEPTH = 64
TILE = 256
STRIP = 128
LAG = 0
SPARE = 8
FIRST_WAIT = 28
SECOND_WAIT = 52
OWN_AT = (0, 4, 8, 12)
PIECE_AT = 4
PIECE_SPAN = 60
BLOCKS = 16

var_floor = 0.05
shrink_level = 0.1


def totals(x):
    middle = middle_sq = None
    for at in range(0, DEPTH, 8):
        if at in (24, 32):
            continue
        part = x[at : at + 8]
        middle = part if middle is None else middle + part
        middle_sq = part * part if middle_sq is None else middle_sq + part * part
    return middle, middle_sq


def day_edges(x, day):
    row = lax.broadcasted_iota(jnp.int32, (8, x.shape[1]), 0)
    newest = jnp.where(row <= day + 4, x[24:32], 0.0)
    oldest = jnp.where(row >= day + 1, x[32:40], 0.0)
    return newest, oldest


def day_moments(x, middle, middle_sq, day):
    newest, oldest = day_edges(x, day)
    total = jnp.sum(middle + newest + oldest, axis=0, keepdims=True)
    total_sq = jnp.sum(middle_sq + newest * newest + oldest * oldest, axis=0, keepdims=True)
    center = total * (1.0 / WIN)
    spread = total_sq * (1.0 / WIN) - center * center
    return center, lax.rsqrt(jnp.maximum(spread, var_floor))


def day_values(x, center, factor, day):
    scaled = (x - center) * factor
    newest, oldest = day_edges(scaled, day)
    return jnp.concatenate([scaled[:24], newest, oldest, scaled[40:]], 0)


def halves(x):
    high = x.astype(jnp.bfloat16)
    low = (x - high.astype(jnp.float32)).astype(jnp.bfloat16)
    return high, low


def odd_place(slot):
    return 1 + slot // 2


def even_place(slot):
    return 9 + slot // 2


def window(store_ref, block, cols):
    x = store_ref[block, 1 : 1 + BLOCKS, :, cols].astype(jnp.float32)
    return x.reshape(DEPTH, TILE)


def kernel(
    returns_ref, signal_ref, earlier_ref, out_ref,
    store_ref, old_ref, before_ref, high_ref, low_ref, bound_ref, lhs_ref, row_ref, sum_ref, lin_ref, x_ref, tot_ref,
    fill_sem, send_far, got_far, send_peer, got_peer, send_edge, got_edge, send_twin, got_twin,
):
    days, mine = out_ref.shape
    time, own = lax.axis_index("tm"), lax.axis_index("asset")
    times, peers = lax.axis_size("tm"), lax.axis_size("asset")
    core = lax.rem(time, 2)
    twin = time + 1 - 2 * core
    even, odd = core == 0, core == 1
    reach = BLOCKS - 1
    column, side = own // 2, lax.rem(own, 2)

    def at(t, a):
        return dict(device_id=(t, a), device_id_type=pl.DeviceIdType.MESH)

    def peer(step, sign):
        along = (0, 0, 1, 3, 2, 1, 3, 2)[step]
        other = (0, 1, 0, 0, 0, 1, 1, 1)[step]
        flipped = 1 - side if other else side
        return 2 * lax.rem(column + (along if sign > 0 else peers // 2 - along), peers // 2) + flipped

    fills = [
        pltpu.make_async_copy(returns_ref, store_ref.at[0, odd_place(reach)], fill_sem.at[0]),
        pltpu.make_async_copy(signal_ref, store_ref.at[0, 0], fill_sem.at[1]),
        pltpu.make_async_copy(earlier_ref, before_ref, fill_sem.at[2]),
    ]
    for fill in fills:
        fill.start()

    barrier = pltpu.get_barrier_semaphore()

    def greet(valid, t, a):
        @pl.when(valid)
        def _():
            pl.semaphore_signal(barrier, inc=1, **at(t, a))

    count = peers
    forward = jnp.logical_and(odd, time + reach < times)
    backward = jnp.logical_and(even, time - reach >= 0)
    greet(forward, time + reach, own)
    greet(backward, time - reach, own)
    count += forward.astype(jnp.int32) + backward.astype(jnp.int32)
    for back in range(reach - 1, 0, -2):
        greet(time + back < times, time + back, own)
        greet(time - back >= 0, time - back, own)
        count += (time + back < times).astype(jnp.int32) + (time - back >= 0).astype(jnp.int32)
    for step in range(1, peers):
        pl.semaphore_signal(barrier, inc=1, **at(time, peer(step, 1)))
    pl.semaphore_signal(barrier, inc=1, **at(twin, own))

    for fill in fills:
        fill.wait()
    shifted = jnp.concatenate(
        [jnp.zeros((1, mine), jnp.float32), before_ref[...].astype(jnp.float32)], 0
    )
    old_ref[...] = shifted.reshape(reach, days, mine).astype(jnp.bfloat16)
    for slot in range(1, reach, 2):
        @pl.when(time + slot < reach)
        def _(slot=slot):
            store_ref[0, odd_place(slot)] = old_ref[time + slot]

    @pl.when(jnp.logical_and(even, time < reach))
    def _():
        store_ref[0, even_place(0)] = old_ref[time]

    sum_ref[...] = jnp.zeros_like(sum_ref)
    lin_ref[...] = jnp.zeros_like(lin_ref)

    pl.semaphore_wait(barrier, count)

    def far(back, place, to):
        return pltpu.make_async_remote_copy(
            src_ref=store_ref.at[0, odd_place(reach)],
            dst_ref=store_ref.at[0, place],
            send_sem=send_far.at[back % reach // 2],
            recv_sem=got_far.at[back % reach // 2],
            **at(to, own),
        )

    @pl.when(forward)
    def _():
        far(reach, even_place(0), time + reach).start()

    for back in range(reach - 1, 0, -2):
        @pl.when(time + back < times)
        def _(back=back):
            far(back, odd_place(reach - back), time + back).start()

    for back in range(2, reach, 2):
        @pl.when(time - back >= 0)
        def _(back=back):
            far(back, odd_place(reach - back), time).wait_recv()

    def across(step, to, held=0):
        half = pl.ds(0, 9)
        return pltpu.make_async_remote_copy(
            src_ref=store_ref.at[held, half],
            dst_ref=store_ref.at[step, half],
            send_sem=send_peer.at[step],
            recv_sem=got_peer.at[step],
            **at(time, to),
        )

    def across_edge(step, to, held=0):
        return pltpu.make_async_remote_copy(
            src_ref=store_ref.at[held, even_place(0) - core],
            dst_ref=store_ref.at[step, even_place(0) + core * SPARE],
            send_sem=send_edge.at[step],
            recv_sem=got_edge.at[step],
            **at(time, to),
        )

    def over(step):
        return pltpu.make_async_remote_copy(
            src_ref=store_ref.at[step, pl.ds(1, 8)],
            dst_ref=store_ref.at[step, pl.ds(9 + core, 8)],
            send_sem=send_twin.at[step],
            recv_sem=got_twin.at[step],
            **at(twin, own),
        )

    def whole(step, edge):
        over(step).wait_recv()
        if edge:
            across_edge(step, own).wait_recv()

    def pass_on(step):
        across(step, own).wait_recv()
        over(step).start()

    over(0).start()
    nearest, opposite, relayed = peers // 2, peers // 2, peers - 1

    for step in range(1, nearest):
        across(step, peer(step, 1)).start()

    @pl.when(backward)
    def _():
        far(reach, even_place(0), time).wait_recv()

    for step in range(1, nearest):
        across_edge(step, peer(step, 1)).start()

    def send_rest():
        for step in range(nearest, relayed):
            across(step, peer(step, 1)).start()
            across_edge(step, peer(step, 1)).start()

    whole(0, False)

    per_block = mine // TILE
    pairs = per_block // 2
    strips = mine // STRIP
    block_steps = days * pairs * strips

    def prepare(block, parity, piece, both_sides=False):
        tile, day = divmod(piece, days)
        cols = pl.ds(tile * TILE, TILE)
        if day == 0:
            x = window(store_ref, block, cols)
            x_ref[tile] = x
            middle, middle_sq = totals(x)
            tot_ref[tile, :8] = middle
            tot_ref[tile, 8:] = middle_sq
        x, middle, middle_sq = x_ref[tile], tot_ref[tile, :8], tot_ref[tile, 8:]
        s = store_ref[block, 0, :, cols].astype(jnp.float32)[day : day + 1]
        center, inverse = day_moments(x, middle, middle_sq, day)
        v = day_values(x, center, inverse * s, day)
        lin_ref[day] += v[:, :128] + v[:, 128:]
        high, low = halves(v)
        high_ref[parity, day, tile] = high
        low_ref[parity, day, tile] = low
        bound_ref[parity, day, tile] = jnp.broadcast_to(jnp.abs(s), (8, TILE))
        if both_sides:
            start = tile * TILE
            w = day_values(x, center, inverse * (1.0 / (WIN * shrink_level)), day)
            row_ref[day, :, start : start + TILE] = w
            high = w.astype(jnp.bfloat16).astype(jnp.float32)
            both = jnp.concatenate([high, w - high], 0)
            for sub in range(0, TILE, 128):
                turned = both[:, sub : sub + 128].T.astype(jnp.bfloat16)
                lhs_ref[day, start + sub : start + sub + 128, :128] = turned
                lhs_ref[day, start + sub : start + sub + 128, 128:] = turned

    pieces = days * per_block

    def compute(*accs):
        def push(parity, place):
            day, pair = divmod(place, pairs)
            for unit in range(2):
                high = high_ref[parity, day, 2 * pair + unit]
                low = low_ref[parity, day, 2 * pair + unit]
                pltpu.matmul_push_rhs(
                    jnp.concatenate([high, high, low, low], 0),
                    staging_register=place % 2,
                    mxu_index=unit,
                )

        def take(parity, step):
            place, strip = divmod(step, strips)
            day, pair = divmod(place, pairs)
            rows = pl.ds(strip * STRIP, STRIP)
            part = None
            for unit in range(2):
                bound = bound_ref[parity, day, 2 * pair + unit][:1]
                got = pltpu.matmul_pop(accs[unit * strips + strip])
                kept = jnp.minimum(jnp.maximum(got, -bound), bound)
                kept = kept[:, :128] + kept[:, 128:]
                part = kept if part is None else part + kept
            sum_ref[day, rows, :] += part

        def steps(parity, first, last, piece_at=None, final=False, begin=False):
            for step in range(first, last):
                place, strip = divmod(step, strips)
                day = place // pairs
                lhs = lhs_ref[day, strip * STRIP : (strip + 1) * STRIP, :]
                for unit in range(2):
                    pltpu.matmul_acc_lhs(
                        accs[unit * strips + strip],
                        lhs,
                        load_staged_rhs=place % 2 if strip == 0 else None,
                    )
                if step >= LAG:
                    take(parity, step - LAG)
                elif not begin:
                    take(1 - parity, block_steps + step - LAG)
                if piece_at is not None:
                    piece_at(step)
                if strip == 0:
                    if step + strips < block_steps:
                        push(parity, place + 1)
                    elif not final:
                        push(1 - parity, 0)

        quarter = block_steps // 4
        for tile in range(per_block):
            prepare(0, 0, tile * days, True)

        def own_pieces(step):
            day, within = divmod(step, quarter)
            for tile in range(per_block):
                if day + 1 < days and within == OWN_AT[tile]:
                    prepare(0, 0, tile * days + day + 1, True)

        push(0, 0)
        steps(0, 0, FIRST_WAIT, own_pieces, begin=True)
        pass_on(1)
        send_rest()
        steps(0, FIRST_WAIT, SECOND_WAIT, own_pieces)
        pass_on(2)
        whole(1, True)

        def first_pieces(step):
            for piece in range(pieces):
                if SECOND_WAIT + piece * (block_steps - SECOND_WAIT - 1) // pieces == step:
                    prepare(1, 1, piece)

        steps(0, SECOND_WAIT, block_steps, first_pieces)

        def one_block(block, carry):
            parity = lax.rem(block, 2)
            whole(block + 1, True)

            @pl.when(block + 2 < peers)
            def _():
                pass_on(block + 2)

            @pl.when(block + 2 == opposite)
            def _():
                across(relayed, peer(1, 1), opposite).start()

            @pl.when(block + 1 == opposite)
            def _():
                across_edge(relayed, peer(1, 1), opposite).start()

            def next_pieces(step):
                for piece in range(pieces):
                    if PIECE_AT + piece * PIECE_SPAN // pieces == step:
                        prepare(block + 1, 1 - parity, piece)

            steps(parity, 0, block_steps, next_pieces)
            return carry

        lax.fori_loop(1, peers - 1, one_block, 0)
        parity = (peers - 1) % 2
        steps(parity, 0, block_steps, final=True)
        for step in range(block_steps - LAG, block_steps):
            take(parity, step)

        for day in range(days):
            weight = jnp.sum(lin_ref[day], axis=1, keepdims=True)
            line = jnp.sum(row_ref[day] * weight, axis=0, keepdims=True)
            clamped = jnp.concatenate(
                [
                    jnp.sum(sum_ref[day, start : start + 128, :].T, axis=0, keepdims=True)
                    for start in range(0, mine, 128)
                ],
                1,
            )
            out_ref[day : day + 1, :] = (line - clamped) * shrink_level

    pl.run_scoped(
        compute,
        *[pltpu.ACC(unit)((STRIP, TILE), jnp.float32) for unit in range(2) for _ in range(strips)],
    )

    @pl.when(forward)
    def _():
        far(reach, even_place(0), time).wait_send()

    for back in range(2, reach, 2):
        @pl.when(time + back < times)
        def _(back=back):
            far(back, odd_place(reach - back), time).wait_send()

    for step in range(peers):
        over(step).wait_send()
        if step:
            across(step, own).wait_send()
            across_edge(step, own).wait_send()


def per_device(returns, signal, earlier):
    days, mine = returns.shape
    peers = lax.axis_size("asset")
    tiles = mine // TILE
    place = pl.BlockSpec(memory_space=pl.ANY)
    vmem, dma = pltpu.VMEM, pltpu.SemaphoreType.DMA
    return pl.pallas_call(
        kernel,
        out_shape=jax.ShapeDtypeStruct((days, mine), jnp.float32),
        in_specs=[place] * 3,
        out_specs=pl.BlockSpec(memory_space=pltpu.VMEM),
        scratch_shapes=[
            vmem((peers, BLOCKS + 2, days, mine), jnp.bfloat16),
            vmem((BLOCKS - 1, days, mine), jnp.bfloat16),
            vmem((HIST, mine), jnp.bfloat16),
            vmem((2, days, tiles, DEPTH, TILE), jnp.bfloat16),
            vmem((2, days, tiles, DEPTH, TILE), jnp.bfloat16),
            vmem((2, days, tiles, 8, TILE), jnp.float32),
            vmem((days, mine, TILE), jnp.bfloat16),
            vmem((days, DEPTH, mine), jnp.float32),
            vmem((days, mine, 128), jnp.float32),
            vmem((days, DEPTH, 128), jnp.float32),
            vmem((tiles, DEPTH, TILE), jnp.float32),
            vmem((tiles, 16, TILE), jnp.float32),
            dma((3,)),
        ]
        + [dma((BLOCKS // 2,))] * 2
        + [dma((peers,))] * 6,
        compiler_params=pltpu.CompilerParams(
            collective_id=0, has_side_effects=True, vmem_limit_bytes=48 << 20
        ),
        name="filter_days",
    )(*(pltpu.with_memory_space_constraint(x, pltpu.HBM) for x in (returns, signal, earlier)))


def solution(mesh):
    in_specs = (P("tm", "asset"), P("tm", "asset"), P(None, "asset"))
    out_specs = P("tm", "asset")
    return jax.shard_map(
        per_device, mesh=mesh, in_specs=in_specs, out_specs=out_specs, check_vma=False
    )
```

```python
import jax
import jax.numpy as jnp
from jax import lax
from jax.experimental import pallas as pl
from jax.experimental.pallas import tpu as pltpu
from jax.sharding import PartitionSpec as P

WIN = 60
HIST = 59
DEPTH = 64
TILE = 256
STRIP = 128
LAG = 0
SPARE = 8
FIRST_WAIT = 28
SECOND_WAIT = 52
OWN_AT = (0, 4, 8, 12)
PIECE_AT = 4
PIECE_SPAN = 60
BLOCKS = 16

var_floor = 0.05
shrink_level = 0.1


def totals(x):
    middle = middle_sq = None
    for at in range(0, DEPTH, 8):
        if at in (24, 32):
            continue
        part = x[at : at + 8]
        middle = part if middle is None else middle + part
        middle_sq = part * part if middle_sq is None else middle_sq + part * part
    return middle, middle_sq


def day_edges(x, day):
    row = lax.broadcasted_iota(jnp.int32, (8, x.shape[1]), 0)
    newest = jnp.where(row <= day + 4, x[24:32], 0.0)
    oldest = jnp.where(row >= day + 1, x[32:40], 0.0)
    return newest, oldest


def day_moments(x, middle, middle_sq, day):
    newest, oldest = day_edges(x, day)
    total = jnp.sum(middle + newest + oldest, axis=0, keepdims=True)
    total_sq = jnp.sum(middle_sq + newest * newest + oldest * oldest, axis=0, keepdims=True)
    center = total * (1.0 / WIN)
    spread = total_sq * (1.0 / WIN) - center * center
    return center, lax.rsqrt(jnp.maximum(spread, var_floor))


def day_values(x, center, factor, day):
    scaled = (x - center) * factor
    newest, oldest = day_edges(scaled, day)
    return jnp.concatenate([scaled[:24], newest, oldest, scaled[40:]], 0)


def halves(x):
    high = x.astype(jnp.bfloat16)
    low = (x - high.astype(jnp.float32)).astype(jnp.bfloat16)
    return high, low


def odd_place(slot):
    return 1 + slot // 2


def even_place(slot):
    return 9 + slot // 2


def window(store_ref, block, cols):
    x = store_ref[block, 1 : 1 + BLOCKS, :, cols].astype(jnp.float32)
    return x.reshape(DEPTH, TILE)


def kernel(
    returns_ref, signal_ref, earlier_ref, out_ref,
    store_ref, old_ref, before_ref, high_ref, low_ref, bound_ref, lhs_ref, row_ref, sum_ref, lin_ref, x_ref, tot_ref,
    fill_sem, send_far, got_far, send_peer, got_peer, send_edge, got_edge, send_twin, got_twin,
):
    days, mine = out_ref.shape
    time, own = lax.axis_index("tm"), lax.axis_index("asset")
    times, peers = lax.axis_size("tm"), lax.axis_size("asset")
    core = lax.rem(time, 2)
    twin = time + 1 - 2 * core
    even, odd = core == 0, core == 1
    reach = BLOCKS - 1
    column, side = own // 2, lax.rem(own, 2)

    def at(t, a):
        return dict(device_id=(t, a), device_id_type=pl.DeviceIdType.MESH)

    def peer(step, sign):
        along = (0, 0, 1, 3, 2, 1, 3, 2)[step]
        other = (0, 1, 0, 0, 0, 1, 1, 1)[step]
        flipped = 1 - side if other else side
        return 2 * lax.rem(column + (along if sign > 0 else peers // 2 - along), peers // 2) + flipped

    fills = [
        pltpu.make_async_copy(returns_ref, store_ref.at[0, odd_place(reach)], fill_sem.at[0]),
        pltpu.make_async_copy(signal_ref, store_ref.at[0, 0], fill_sem.at[1]),
        pltpu.make_async_copy(earlier_ref, before_ref, fill_sem.at[2]),
    ]
    for fill in fills:
        fill.start()

    barrier = pltpu.get_barrier_semaphore()

    def greet(valid, t, a):
        @pl.when(valid)
        def _():
            pl.semaphore_signal(barrier, inc=1, **at(t, a))

    count = peers
    forward = jnp.logical_and(odd, time + reach < times)
    backward = jnp.logical_and(even, time - reach >= 0)
    greet(forward, time + reach, own)
    greet(backward, time - reach, own)
    count += forward.astype(jnp.int32) + backward.astype(jnp.int32)
    for back in range(reach - 1, 0, -2):
        greet(time + back < times, time + back, own)
        greet(time - back >= 0, time - back, own)
        count += (time + back < times).astype(jnp.int32) + (time - back >= 0).astype(jnp.int32)
    for step in range(1, peers):
        pl.semaphore_signal(barrier, inc=1, **at(time, peer(step, 1)))
    pl.semaphore_signal(barrier, inc=1, **at(twin, own))

    for fill in fills:
        fill.wait()
    shifted = jnp.concatenate(
        [jnp.zeros((1, mine), jnp.float32), before_ref[...].astype(jnp.float32)], 0
    )
    old_ref[...] = shifted.reshape(reach, days, mine).astype(jnp.bfloat16)
    for slot in range(1, reach, 2):
        @pl.when(time + slot < reach)
        def _(slot=slot):
            store_ref[0, odd_place(slot)] = old_ref[time + slot]

    @pl.when(jnp.logical_and(even, time < reach))
    def _():
        store_ref[0, even_place(0)] = old_ref[time]

    sum_ref[...] = jnp.zeros_like(sum_ref)
    lin_ref[...] = jnp.zeros_like(lin_ref)

    pl.semaphore_wait(barrier, count)

    def far(back, place, to):
        return pltpu.make_async_remote_copy(
            src_ref=store_ref.at[0, odd_place(reach)],
            dst_ref=store_ref.at[0, place],
            send_sem=send_far.at[back % reach // 2],
            recv_sem=got_far.at[back % reach // 2],
            **at(to, own),
        )

    @pl.when(forward)
    def _():
        far(reach, even_place(0), time + reach).start()

    for back in range(reach - 1, 0, -2):
        @pl.when(time + back < times)
        def _(back=back):
            far(back, odd_place(reach - back), time + back).start()

    for back in range(2, reach, 2):
        @pl.when(time - back >= 0)
        def _(back=back):
            far(back, odd_place(reach - back), time).wait_recv()

    def across(step, to, held=0):
        half = pl.ds(0, 9)
        return pltpu.make_async_remote_copy(
            src_ref=store_ref.at[held, half],
            dst_ref=store_ref.at[step, half],
            send_sem=send_peer.at[step],
            recv_sem=got_peer.at[step],
            **at(time, to),
        )

    def across_edge(step, to, held=0):
        return pltpu.make_async_remote_copy(
            src_ref=store_ref.at[held, even_place(0) - core],
            dst_ref=store_ref.at[step, even_place(0) + core * SPARE],
            send_sem=send_edge.at[step],
            recv_sem=got_edge.at[step],
            **at(time, to),
        )

    def over(step):
        return pltpu.make_async_remote_copy(
            src_ref=store_ref.at[step, pl.ds(1, 8)],
            dst_ref=store_ref.at[step, pl.ds(9 + core, 8)],
            send_sem=send_twin.at[step],
            recv_sem=got_twin.at[step],
            **at(twin, own),
        )

    def whole(step, edge):
        over(step).wait_recv()
        if edge:
            across_edge(step, own).wait_recv()

    def pass_on(step):
        across(step, own).wait_recv()
        over(step).start()

    over(0).start()
    nearest, opposite, relayed = peers // 2, peers // 2, peers - 1

    for step in range(1, nearest):
        across(step, peer(step, 1)).start()

    @pl.when(backward)
    def _():
        far(reach, even_place(0), time).wait_recv()

    for step in range(1, nearest):
        across_edge(step, peer(step, 1)).start()

    def send_rest():
        for step in range(nearest, relayed):
            across(step, peer(step, 1)).start()
            across_edge(step, peer(step, 1)).start()

    whole(0, False)

    per_block = mine // TILE
    pairs = per_block // 2
    strips = mine // STRIP
    block_steps = days * pairs * strips

    def prepare(block, parity, piece, both_sides=False):
        tile, day = divmod(piece, days)
        cols = pl.ds(tile * TILE, TILE)
        if day == 0:
            x = window(store_ref, block, cols)
            x_ref[tile] = x
            middle, middle_sq = totals(x)
            tot_ref[tile, :8] = middle
            tot_ref[tile, 8:] = middle_sq
        x, middle, middle_sq = x_ref[tile], tot_ref[tile, :8], tot_ref[tile, 8:]
        s = store_ref[block, 0, :, cols].astype(jnp.float32)[day : day + 1]
        center, inverse = day_moments(x, middle, middle_sq, day)
        v = day_values(x, center, inverse * s, day)
        lin_ref[day] += v[:, :128] + v[:, 128:]
        high, low = halves(v)
        high_ref[parity, day, tile] = high
        low_ref[parity, day, tile] = low
        bound_ref[parity, day, tile] = jnp.broadcast_to(jnp.abs(s), (8, TILE))
        if both_sides:
            start = tile * TILE
            w = day_values(x, center, inverse * (1.0 / (WIN * shrink_level)), day)
            row_ref[day, :, start : start + TILE] = w
            high = w.astype(jnp.bfloat16).astype(jnp.float32)
            both = jnp.concatenate([high, w - high], 0)
            for sub in range(0, TILE, 128):
                turned = both[:, sub : sub + 128].T.astype(jnp.bfloat16)
                lhs_ref[day, start + sub : start + sub + 128, :128] = turned
                lhs_ref[day, start + sub : start + sub + 128, 128:] = turned

    pieces = days * per_block

    def compute(*accs):
        def push(parity, place):
            day, pair = divmod(place, pairs)
            for unit in range(2):
                high = high_ref[parity, day, 2 * pair + unit]
                low = low_ref[parity, day, 2 * pair + unit]
                pltpu.matmul_push_rhs(
                    jnp.concatenate([high, high, low, low], 0),
                    staging_register=place % 2,
                    mxu_index=unit,
                )

        def take(parity, step):
            place, strip = divmod(step, strips)
            day, pair = divmod(place, pairs)
            rows = pl.ds(strip * STRIP, STRIP)
            part = None
            for unit in range(2):
                bound = bound_ref[parity, day, 2 * pair + unit][:1]
                got = pltpu.matmul_pop(accs[unit * strips + strip])
                kept = jnp.minimum(jnp.maximum(got, -bound), bound)
                kept = kept[:, :128] + kept[:, 128:]
                part = kept if part is None else part + kept
            sum_ref[day, rows, :] += part

        def steps(parity, first, last, piece_at=None, final=False, begin=False):
            for step in range(first, last):
                place, strip = divmod(step, strips)
                day = place // pairs
                lhs = lhs_ref[day, strip * STRIP : (strip + 1) * STRIP, :]
                for unit in range(2):
                    pltpu.matmul_acc_lhs(
                        accs[unit * strips + strip],
                        lhs,
                        load_staged_rhs=place % 2 if strip == 0 else None,
                    )
                if step >= LAG:
                    take(parity, step - LAG)
                elif not begin:
                    take(1 - parity, block_steps + step - LAG)
                if piece_at is not None:
                    piece_at(step)
                if strip == 0:
                    if step + strips < block_steps:
                        push(parity, place + 1)
                    elif not final:
                        push(1 - parity, 0)

        quarter = block_steps // 4
        for tile in range(per_block):
            prepare(0, 0, tile * days, True)

        def own_pieces(step):
            day, within = divmod(step, quarter)
            for tile in range(per_block):
                if day + 1 < days and within == OWN_AT[tile]:
                    prepare(0, 0, tile * days + day + 1, True)

        push(0, 0)
        steps(0, 0, FIRST_WAIT, own_pieces, begin=True)
        pass_on(1)
        pass_on(2)
        send_rest()
        steps(0, FIRST_WAIT, SECOND_WAIT, own_pieces)
        whole(1, True)

        def first_pieces(step):
            for piece in range(pieces):
                if SECOND_WAIT + piece * (block_steps - SECOND_WAIT - 1) // pieces == step:
                    prepare(1, 1, piece)

        steps(0, SECOND_WAIT, block_steps, first_pieces)

        def one_block(block, carry):
            parity = lax.rem(block, 2)
            whole(block + 1, True)

            @pl.when(block + 2 < peers)
            def _():
                pass_on(block + 2)

            @pl.when(block + 2 == opposite)
            def _():
                across(relayed, peer(1, 1), opposite).start()

            @pl.when(block + 1 == opposite)
            def _():
                across_edge(relayed, peer(1, 1), opposite).start()

            def next_pieces(step):
                for piece in range(pieces):
                    if PIECE_AT + piece * PIECE_SPAN // pieces == step:
                        prepare(block + 1, 1 - parity, piece)

            steps(parity, 0, block_steps, next_pieces)
            return carry

        lax.fori_loop(1, peers - 1, one_block, 0)
        parity = (peers - 1) % 2
        steps(parity, 0, block_steps, final=True)
        for step in range(block_steps - LAG, block_steps):
            take(parity, step)

        for day in range(days):
            weight = jnp.sum(lin_ref[day], axis=1, keepdims=True)
            line = jnp.sum(row_ref[day] * weight, axis=0, keepdims=True)
            clamped = jnp.concatenate(
                [
                    jnp.sum(sum_ref[day, start : start + 128, :].T, axis=0, keepdims=True)
                    for start in range(0, mine, 128)
                ],
                1,
            )
            out_ref[day : day + 1, :] = (line - clamped) * shrink_level

    pl.run_scoped(
        compute,
        *[pltpu.ACC(unit)((STRIP, TILE), jnp.float32) for unit in range(2) for _ in range(strips)],
    )

    @pl.when(forward)
    def _():
        far(reach, even_place(0), time).wait_send()

    for back in range(2, reach, 2):
        @pl.when(time + back < times)
        def _(back=back):
            far(back, odd_place(reach - back), time).wait_send()

    for step in range(peers):
        over(step).wait_send()
        if step:
            across(step, own).wait_send()
            across_edge(step, own).wait_send()


def per_device(returns, signal, earlier):
    days, mine = returns.shape
    peers = lax.axis_size("asset")
    tiles = mine // TILE
    place = pl.BlockSpec(memory_space=pl.ANY)
    vmem, dma = pltpu.VMEM, pltpu.SemaphoreType.DMA
    return pl.pallas_call(
        kernel,
        out_shape=jax.ShapeDtypeStruct((days, mine), jnp.float32),
        in_specs=[place] * 3,
        out_specs=pl.BlockSpec(memory_space=pltpu.VMEM),
        scratch_shapes=[
            vmem((peers, BLOCKS + 2, days, mine), jnp.bfloat16),
            vmem((BLOCKS - 1, days, mine), jnp.bfloat16),
            vmem((HIST, mine), jnp.bfloat16),
            vmem((2, days, tiles, DEPTH, TILE), jnp.bfloat16),
            vmem((2, days, tiles, DEPTH, TILE), jnp.bfloat16),
            vmem((2, days, tiles, 8, TILE), jnp.float32),
            vmem((days, mine, TILE), jnp.bfloat16),
            vmem((days, DEPTH, mine), jnp.float32),
            vmem((days, mine, 128), jnp.float32),
            vmem((days, DEPTH, 128), jnp.float32),
            vmem((tiles, DEPTH, TILE), jnp.float32),
            vmem((tiles, 16, TILE), jnp.float32),
            dma((3,)),
        ]
        + [dma((BLOCKS // 2,))] * 2
        + [dma((peers,))] * 6,
        compiler_params=pltpu.CompilerParams(
            collective_id=0, has_side_effects=True, vmem_limit_bytes=48 << 20
        ),
        name="filter_days",
    )(*(pltpu.with_memory_space_constraint(x, pltpu.HBM) for x in (returns, signal, earlier)))


def solution(mesh):
    in_specs = (P("tm", "asset"), P("tm", "asset"), P(None, "asset"))
    out_specs = P("tm", "asset")
    return jax.shard_map(
        per_device, mesh=mesh, in_specs=in_specs, out_specs=out_specs, check_vma=False
    )
```
